32 devices in a mesh: data: 32 (over z, y, x, core).
Axes of the slice: x: 2, y: 2, z: 4, core: 2. Of those that a mesh axis runs over, the one named last changes fastest.
Arguments:
- tokens: bfloat16 [65536, 1280], P('data')
- w_up: bfloat16 [1280, 5120], replicated
- w_down: bfloat16 [5120, 1280], replicated
- heads: bfloat16 [8, 1280, 2], replicated
- labels: int32 [8, 65536], P(None, 'data')
Outputs:
- output 1: float32 [8], replicated
- output 2: float32 [1280, 5120], P('data')
- output 3: float32 [5120, 1280], P('data')
All inputs are finite; a program needn't handle non-finite values.
Results may differ from the reference program's by a relative error of at most 0.00256343.
Values are sent between devices in bfloat16 or wider.
A program may use at most 1 GiB of HBM per device.

```python
import jax
import jax.numpy as jnp
from jax import lax

MODEL_DIM = 1280
HIDDEN_DIM = 5120
NUM_TASKS = 8
NUM_CLASSES = 2
TOKENS_DEV = 2048
GROUP_SIZE = 32
SOLVER_STEPS = 20


def draw_labels(label_key):
    label_keys = jax.random.split(label_key, 4)
    total_rows = TOKENS_DEV * GROUP_SIZE
    spread = (NUM_CLASSES + 1) // 2
    offsets = jax.random.randint(label_keys[0], (GROUP_SIZE,), 0, NUM_CLASSES)
    shared = (jnp.repeat(offsets, TOKENS_DEV) + jax.random.randint(label_keys[1], (total_rows,), 0, spread)) % NUM_CLASSES
    keep_mask = jax.random.randint(label_keys[2], (NUM_TASKS, total_rows), 0, 10) < 7
    own_labels = jax.random.randint(label_keys[3], (NUM_TASKS, total_rows), 0, NUM_CLASSES)
    return jnp.where(keep_mask, shared[None, :], own_labels).astype(jnp.int32)


def setup_inputs(seed: int = 0) -> dict:
    root_key = jax.random.key(seed)
    sub_keys = jax.random.split(root_key, 7)
    total_rows = TOKENS_DEV * GROUP_SIZE
    tokens = jax.random.normal(sub_keys[0], (total_rows, MODEL_DIM), jnp.float32)
    w_up = jax.random.normal(sub_keys[1], (MODEL_DIM, HIDDEN_DIM), jnp.float32) * MODEL_DIM ** -0.5
    w_down = jax.random.normal(sub_keys[2], (HIDDEN_DIM, MODEL_DIM), jnp.float32) * HIDDEN_DIM ** -0.5
    shared_head = jax.random.normal(sub_keys[3], (1, MODEL_DIM, NUM_CLASSES), jnp.float32)
    own_head = jax.random.normal(sub_keys[4], (NUM_TASKS, MODEL_DIM, NUM_CLASSES), jnp.float32)
    task_scale = jax.random.uniform(sub_keys[5], (NUM_TASKS, 1, 1), jnp.float32, 0.7, 1.3)
    signs = (1 - 2 * (jnp.arange(NUM_TASKS) % 2)).astype(jnp.float32).reshape(NUM_TASKS, 1, 1)
    heads = task_scale * (0.8 * signs * shared_head + 0.6 * own_head) * MODEL_DIM ** -0.5
    labels = draw_labels(sub_keys[6])
    return {'tokens': tokens.astype(jnp.bfloat16), 'w_up': w_up.astype(jnp.bfloat16), 'w_down': w_down.astype(jnp.bfloat16), 'heads': heads.astype(jnp.bfloat16), 'labels': labels}


def trunk_forward(x_rows, w_up, w_down):
    pre_act = jnp.dot(x_rows, w_up, preferred_element_type=jnp.float32).astype(jnp.bfloat16)
    hidden = jax.nn.gelu(pre_act.astype(jnp.float32)).astype(jnp.bfloat16)
    trunk_out = x_rows.astype(jnp.float32) + jnp.dot(hidden, w_down, preferred_element_type=jnp.float32)
    return pre_act, hidden, trunk_out


def task_residuals(trunk_out, heads_f32, label_rows, total_rows):
    logits = jnp.einsum('bd,tdc->tbc', trunk_out.astype(jnp.bfloat16).astype(jnp.float32), heads_f32)
    onehot = (label_rows[:, :, None] == jnp.arange(NUM_CLASSES)[None, None, :]).astype(jnp.float32)
    return (jax.nn.softmax(logits, axis=-1) - onehot) / total_rows


def solve_weights(full_gram):
    step_scale = jnp.trace(full_gram) / NUM_TASKS

    def update(step_idx, mix_wts):
        descent = jnp.sum(full_gram * mix_wts[None, :], axis=1)
        mix_wts = mix_wts * jnp.exp(-descent / step_scale)
        return mix_wts / jnp.sum(mix_wts)

    uniform_start = jnp.full((NUM_TASKS,), 1.0 / NUM_TASKS, jnp.float32)
    return lax.fori_loop(0, SOLVER_STEPS, update, uniform_start)


def reference(tokens, w_up, w_down, heads, labels):
    total_rows = tokens.shape[0]
    num_blocks = total_rows // TOKENS_DEV
    tok_blocks = tokens.reshape(num_blocks, TOKENS_DEV, MODEL_DIM)
    lab_blocks = labels.reshape(NUM_TASKS, num_blocks, TOKENS_DEV).transpose(1, 0, 2)
    heads_f32 = heads.astype(jnp.float32)
    head_gram = jnp.einsum('tdc,sde->tcse', heads_f32, heads_f32)

    def gram_step(gram_acc, block_in):
        x_rows, label_rows = block_in
        trunk_out = trunk_forward(x_rows, w_up, w_down)[2]
        task_resid = task_residuals(trunk_out, heads_f32, label_rows, total_rows)
        res_outer = jnp.einsum('tbc,sbe->tcse', task_resid, task_resid)
        return gram_acc + jnp.sum(res_outer * head_gram, axis=(1, 3)), None

    full_gram, _ = lax.scan(gram_step, jnp.zeros((NUM_TASKS, NUM_TASKS), jnp.float32), (tok_blocks, lab_blocks))
    mix_weights = solve_weights(full_gram)

    def grad_step(grad_acc, block_in):
        x_rows, label_rows = block_in
        pre_act, hidden, trunk_out = trunk_forward(x_rows, w_up, w_down)
        task_resid = task_residuals(trunk_out, heads_f32, label_rows, total_rows)
        d_out = jnp.einsum('tbc,tdc->bd', task_resid * mix_weights[:, None, None], heads_f32).astype(jnp.bfloat16)
        grad_down = jnp.dot(hidden.T, d_out, preferred_element_type=jnp.float32)
        d_hidden = jnp.dot(d_out, w_down.T, preferred_element_type=jnp.float32)
        gelu_vjp = jax.vjp(jax.nn.gelu, pre_act.astype(jnp.float32))[1]
        d_pre = gelu_vjp(d_hidden)[0].astype(jnp.bfloat16)
        grad_up = jnp.dot(x_rows.T, d_pre, preferred_element_type=jnp.float32)
        return (grad_acc[0] + grad_up, grad_acc[1] + grad_down), None

    zero_grads = (jnp.zeros((MODEL_DIM, HIDDEN_DIM), jnp.float32), jnp.zeros((HIDDEN_DIM, MODEL_DIM), jnp.float32))
    (grad_up, grad_down), _ = lax.scan(grad_step, zero_grads, (tok_blocks, lab_blocks))
    return mix_weights, grad_up, grad_down
```

```python
import functools
import math

import jax
import jax.numpy as jnp
from jax import lax
from jax.experimental import pallas as pl
from jax.experimental.pallas import tpu as pltpu
from jax.sharding import PartitionSpec as P

F32 = jnp.float32
BF16 = jnp.bfloat16
MESH = pl.DeviceIdType.MESH
SOLVER_STEPS = 20
NUM_TASKS = 8
NUM_DEV = 32
NUM_CHIPS = 16
TOK = 2048
PAIR_TOK = 4096
DIM = 1280
HID = 5120
HALF = 2560
TB = 512
NTB = PAIR_TOK // TB
CW = 256
NBLK = HALF // CW
ROWS = 80
C0 = math.sqrt(2.0 / math.pi)
C1 = C0 * 0.044715


def split3(v):
    hi = v.astype(BF16)
    rem = v - hi.astype(F32)
    mid = rem.astype(BF16)
    lo = (rem - mid.astype(F32)).astype(BF16)
    return hi, mid, lo


def dot(a, b, dims=((1,), (0,))):
    return lax.dot_general(a, b, (dims, ((), ())), preferred_element_type=F32)


def remote(src, dst, ssem, rsem, dev):
    return pltpu.make_async_remote_copy(
        src_ref=src, dst_ref=dst, send_sem=ssem, recv_sem=rsem,
        device_id=(dev,), device_id_type=MESH)


def sublane_sum(v):
    for sh in (4, 2, 1):
        v = v + pltpu.roll(v, sh, 0)
    return v


def rolled(v, k):
    return v if k == 0 else pltpu.roll(v, NUM_TASKS - k, 0)


def kernel(x_hbm, w1_hbm, w2_hbm, hc_ref, lab_ref,
           mix_ref, up_hbm, down_ref, a_hbm, xs_hbm,
           wbuf, w1, xt, abuf, gs, gt, agt, dpc, st, st_in, lab_in, rs, r3, tref, tp, trecv, mrecv,
           gbuf, q1, q2, q3, fin,
           wsem, w1sem, xsem, asem, ainsem, pair_s, pair_r, msend, mrec, tsend, trec,
           s1, v1, s2, v2, s3, v3, fs_loc, fs, fv):
    me = lax.axis_index("data")
    core = lax.rem(me, 2)
    chip = me // 2
    cx = lax.rem(chip, 2)
    cy = lax.rem(chip // 2, 2)
    cz = chip // 4
    sib = me + 1 - 2 * core

    def w2_load(c):
        return pltpu.make_async_copy(w2_hbm.at[pl.ds(pl.multiple_of(core * HALF + c * TB, TB), TB)], wbuf.at[c], wsem.at[c])

    def w1_load(c):
        return pltpu.make_async_copy(
            w1_hbm.at[:, pl.ds(pl.multiple_of(core * HALF + c * TB, TB), TB)], w1.at[:, pl.ds(c * TB, TB)], w1sem.at[c])

    def x_load_own(i, slot):
        return pltpu.make_async_copy(x_hbm.at[pl.ds(pl.multiple_of(i * TB, TB), TB)], wbuf.at[slot], xsem.at[slot])

    def x_load_sib(i, slot):
        return pltpu.make_async_copy(xs_hbm.at[pl.ds(pl.multiple_of((i - 4) * TB, TB), TB)], wbuf.at[slot], xsem.at[slot])

    for c in range(5):
        w2_load(c).start()
    for c in range(5):
        w1_load(c).start()

    barrier = pltpu.get_barrier_semaphore()
    for m in range(1, NUM_DEV):
        pl.semaphore_signal(barrier, inc=1, device_id=(lax.rem(me + m, NUM_DEV),), device_id_type=MESH)

    hc = hc_ref[...]
    diff = hc[:NUM_TASKS].astype(F32) - hc[NUM_TASKS:].astype(F32)
    dpieces = jnp.concatenate([p.astype(F32) for p in split3(diff)] + [jnp.zeros((104, DIM), F32)], axis=0)
    dpc[...] = dpieces.T.astype(BF16)
    for c in range(5):
        w2_load(c).wait()
        g24 = dot(wbuf[c], dpc[...])
        if c < 4:
            x_load_own(c, c).start()
        g24t = g24.T
        g8 = g24t[0:8] + g24t[8:16] + g24t[16:24]
        gt[:, c * TB:(c + 1) * TB] = g8
        pieces = jnp.concatenate([p.astype(F32) for p in split3(g8)] + [jnp.zeros((104, TB), F32)], axis=0)
        gs[c * TB:(c + 1) * TB, :] = pieces.T.astype(BF16)

    pl.semaphore_wait(barrier, NUM_DEV - 1)
    x_pair = remote(x_hbm, xs_hbm, pair_s.at[0], pair_r.at[0], sib)
    x_pair.start()
    lab_pair = remote(lab_ref, lab_in, pair_s.at[1], pair_r.at[1], sib)
    lab_pair.start()
    for c in range(5):
        w1_load(c).wait()

    def a_store(par, nb, at):
        return pltpu.make_async_copy(abuf.at[par * NBLK + nb], a_hbm.at[nb, at], asem.at[par, nb])

    def fwd(i, carry):
        slot = lax.rem(i, 5)
        par = lax.rem(i, 2)
        at = lax.rem(core * 4 + i, 8)
        col = pl.multiple_of(at * TB, TB)

        @pl.when(i == 3)
        def _():
            x_pair.wait_recv()

        @pl.when((i >= 3) & (i < 7))
        def _():
            x_load_sib(i + 1, lax.rem(i + 1, 5)).start()

        x_load_own(0, slot).wait()

        @pl.when(i >= 2)
        def _():
            for nb in range(NBLK):
                a_store(par, nb, at).wait()

        xb = wbuf[slot]
        total = None
        for t in range(5):
            pre = dot(xb, w1[:, t * TB:(t + 1) * TB]).astype(BF16)
            abuf[par * NBLK + 2 * t] = pre[:, :CW]
            abuf[par * NBLK + 2 * t + 1] = pre[:, CW:]
            af = pre.astype(F32)
            th = jnp.tanh(af * (C0 + C1 * (af * af)))
            h = 0.5 * af
            pb = (h + h * th).astype(BF16)
            part = dot(pb, gs[t * TB:(t + 1) * TB, :])
            total = part if total is None else total + part
        for nb in range(NBLK):
            a_store(par, nb, at).start()
        xbt = xb.T
        for c in range(NUM_CHIPS):
            zz, yy, xx = c // 4, (c // 2) % 2, c % 2
            xt[xx, yy, zz * ROWS:(zz + 1) * ROWS, pl.ds(col, TB)] = xbt[c * ROWS:(c + 1) * ROWS]
        tt = total.T
        st[:, pl.ds(col, TB)] = tt[0:8] + tt[8:16] + tt[16:24]

        @pl.when(i < 4)
        def _():
            xd = dot(wbuf[slot], dpc[...]).T
            st[:, pl.ds(col, TB)] += xd[0:8] + xd[8:16] + xd[16:24]

        return carry

    lax.fori_loop(0, NTB, fwd, 0)
    for par in range(2):
        for nb in range(NBLK):
            a_store(par, nb, 0).wait()

    st_pair = remote(st, st_in, pair_s.at[2], pair_r.at[2], sib)
    st_pair.start()

    def a_load(j):
        return pltpu.make_async_copy(
            a_hbm.at[j], abuf.at[pl.ds(pl.multiple_of(lax.rem(j, 2) * 8, 8), 8)], ainsem.at[lax.rem(j, 2)])

    a_load(0).start()
    lane = lax.broadcasted_iota(jnp.int32, (NUM_TASKS, 128), 1)
    dgram = jnp.zeros((NUM_TASKS, 128), F32)
    for k in range(NUM_TASKS):
        dgram = jnp.where(lane == k, jnp.sum(diff * rolled(diff, k), axis=1, keepdims=True), dgram)
    lab_pair.wait_recv()
    st_pair.wait_recv()
    own_col = pl.multiple_of(core * TOK, TOK)
    sib_col = pl.multiple_of((1 - core) * TOK, TOK)

    def resid(col, labels):
        delta = st[:, pl.ds(col, TOK)] + st_in[:, pl.ds(col, TOK)]
        sign = jnp.where(labels == 0, -1.0, 1.0)
        u = sign * delta
        e = jnp.exp(-jnp.abs(u))
        return sign * (jnp.where(u >= 0, 1.0, e) / (1.0 + e)) * (1.0 / (TOK * NUM_DEV))

    ra = resid(own_col, lab_ref[...])
    rb = resid(sib_col, lab_in[...])
    first = core == 0
    rlo = jnp.where(first, ra, rb)
    rhi = jnp.where(first, rb, ra)
    cg = jnp.zeros((NUM_TASKS, 128), F32)
    for k in range(NUM_TASKS):
        prod = rlo * rolled(rlo, k) + rhi * rolled(rhi, k)
        cg = jnp.where(lane == k, jnp.sum(prod, axis=1, keepdims=True), cg)
    mrecv[chip] = cg

    def m_copy(m):
        dst = lax.rem(chip + m, NUM_CHIPS) * 2 + core
        return remote(mrecv.at[chip], mrecv.at[chip], msend.at[m - 1], mrec.at[m - 1], dst)

    for m in range(1, NUM_CHIPS):
        m_copy(m).start()

    for part, r in ((0, rlo), (1, rhi)):
        hi, mid, lo = split3(r)
        base = part * TOK
        r3[:, base:base + TOK] = jnp.concatenate([hi.astype(F32), mid.astype(F32), lo.astype(F32), jnp.zeros_like(r)], axis=0).astype(BF16)
        hf, mf, lf = hi.astype(F32), mid.astype(F32), lo.astype(F32)
        for c in range(TOK // TB):
            sl = slice(c * TB, (c + 1) * TB)
            stack = jnp.concatenate([hf[:, sl], hf[:, sl], mf[:, sl], hf[:, sl], lf[:, sl], mf[:, sl], jnp.zeros((80, TB), F32)], axis=0)
            rs[base + c * TB:base + (c + 1) * TB, :] = stack.T.astype(BF16)

    for m in range(1, NUM_CHIPS):
        m_copy(m).wait_recv()
    mp = mrecv[0]
    for c in range(1, NUM_CHIPS):
        mp = mp + mrecv[c]
    mp = mp * dgram
    cols = [jnp.broadcast_to(mp[:, k:k + 1], (NUM_TASKS, 128)) for k in range(NUM_TASKS)]
    inv_scale = NUM_TASKS / sublane_sum(cols[0])

    def solve(step, w):
        ws = [rolled(w, k) for k in range(NUM_TASKS)]
        prods = [cols[k] * ws[k] for k in range(NUM_TASKS)]
        while len(ws) > 1:
            ws = [ws[i] + ws[i + 1] for i in range(0, len(ws), 2)]
            prods = [prods[i] + prods[i + 1] for i in range(0, len(prods), 2)]
        inv = 1.0 / ws[0]
        return (w * inv) * jnp.exp(-(prods[0] * inv) * inv_scale)

    wts = lax.fori_loop(0, SOLVER_STEPS, solve, jnp.full((NUM_TASKS, 128), 1.0 / NUM_TASKS, F32))
    wts = wts / sublane_sum(wts)
    mix_ref[...] = wts
    wcol = wts[:, 0:1]
    hi, mid, lo = [p.astype(F32) for p in split3(gt[...] * wcol)]
    agt[...] = jnp.concatenate([hi, mid, hi, lo, hi, mid, jnp.zeros((80, HALF), F32)], axis=0).astype(BF16)

    def order(j):
        odd = lax.rem(j, 2)
        p1 = (1 - odd) * cx + odd * cy
        p2 = (1 - odd) * cy + odd * cx
        dx = me + 2 * (1 - 2 * cx)
        dy = me + 4 * (1 - 2 * cy)
        return odd, p1, p2, (1 - odd) * dx + odd * dy, (1 - odd) * dy + odd * dx

    def copy1(j):
        odd, p1, p2, d1, d2 = order(j)
        return remote(gbuf.at[j, 1 - p1], q1.at[j], s1.at[j], v1.at[j], d1)

    def copy2(j):
        odd, p1, p2, d1, d2 = order(j)
        return remote(gbuf.at[j, p1, 1 - p2], q2.at[j], s2.at[j], v2.at[j], d2)

    def copy3(j, m):
        odd, p1, p2, d1, d2 = order(j)
        z2 = lax.rem(cz + m, 4)
        dst = z2 * 8 + cy * 4 + cx * 2 + core
        return remote(gbuf.at[j, p1, p2, z2], q3.at[j, m - 1], s3.at[j, m - 1], v3.at[j, m - 1], dst)

    def out_cols(j):
        return pl.ds(pl.multiple_of(core * HALF + j * CW, CW), CW)

    def out_local(j):
        return pltpu.make_async_copy(fin.at[j, core], up_hbm.at[:, out_cols(j)], fs_loc.at[j])

    def out_pair(j):
        return remote(fin.at[j, 1 - core], up_hbm.at[:, out_cols(j)], fs.at[j], fv.at[j], sib)

    def stage2(j):
        odd, p1, p2, d1, d2 = order(j)
        copy1(j).wait_recv()
        gbuf[j, p1, 1 - p2] += q1[j, 1 - p2]
        copy2(j).start()
        gbuf[j, p1, p2] += q1[j, p2]

    def stage3(j):
        odd, p1, p2, d1, d2 = order(j)
        copy2(j).wait_recv()
        gbuf[j, p1, p2] += q2[j]
        for m in (2, 1, 3):
            copy3(j, m).start()

    def finish(j):
        odd, p1, p2, d1, d2 = order(j)
        for m in (1, 2, 3):
            copy3(j, m).wait_recv()
        tot = gbuf[j, p1, p2, cz] + q3[j, 0] + q3[j, 1] + q3[j, 2]
        fin[j, 0] = tot[:ROWS // 2]
        fin[j, 1] = tot[ROWS // 2:]
        out_local(j).start()
        out_pair(j).start()

    def block(j, carry):
        odd, p1, p2, d1, d2 = order(j)
        a_load(j).wait()

        @pl.when(j < NBLK - 1)
        def _():
            a_load(j + 1).start()

        jcol = pl.multiple_of(j * CW, CW)
        base = lax.rem(j, 2) * 8

        def elem(tb, tacc):
            row = pl.multiple_of(tb * TB, TB)
            af = abuf[base + tb].astype(F32)
            dp = dot(rs[pl.ds(row, TB), :], agt[:, pl.ds(jcol, CW)])
            a2 = af * af
            th = jnp.tanh(af * (C0 + C1 * a2))
            h = 0.5 * af
            pb = (h + h * th).astype(BF16)
            slope = (0.5 + 0.5 * th) + (h * (1.0 - th * th)) * (C0 + (3.0 * C1) * a2)
            abuf[16 + tb] = (dp * slope).astype(BF16)
            return tacc + dot(r3[:, pl.ds(row, TB)], pb)

        tacc = lax.fori_loop(0, NTB, elem, jnp.zeros((32, CW), F32))
        tref[:, pl.ds(jcol, CW)] = tacc[0:8] + tacc[8:16] + tacc[16:24]

        def chunk(q, c2):
            a1 = q // 2
            b1 = lax.rem(q, 2)
            i1 = (1 - a1) * (1 - p1) + a1 * p1
            xi = (1 - odd) * i1 + odd * b1
            yi = (1 - odd) * b1 + odd * i1
            g = dot(xt[xi, yi], abuf[16:24].reshape(PAIR_TOK, CW))
            gbuf[j, i1, b1] = g.reshape(4, ROWS, CW)

            @pl.when(q == 1)
            def _():
                copy1(j).start()

            return c2

        lax.fori_loop(0, 4, chunk, 0)

        @pl.when(j >= 1)
        def _():
            stage2(j - 1)

        @pl.when(j >= 2)
        def _():
            stage3(j - 2)

        @pl.when(j >= 3)
        def _():
            finish(j - 3)

        return carry

    lax.fori_loop(0, NBLK, block, 0)

    for i in range(NUM_CHIPS):
        tp[i, :, 0:160] = tref[:, i * 160:(i + 1) * 160]

    def t_copy(i, src_chip):
        return remote(tp.at[i], trecv.at[src_chip], tsend.at[i], trec.at[src_chip], core * 16 + i)

    for i in range(NUM_CHIPS):
        @pl.when(core * 16 + i != me)
        def _():
            t_copy(i, chip).start()

        @pl.when(core * 16 + i == me)
        def _():
            trecv[chip] = tp[i]

    stage2(NBLK - 1)
    stage3(NBLK - 2)
    finish(NBLK - 3)

    for c in range(NUM_CHIPS):
        @pl.when(c * 2 + me // 16 != me)
        def _():
            t_copy(0, c).wait_recv()

    tsum = trecv[0]
    for c in range(1, NUM_CHIPS):
        tsum = tsum + trecv[c]
    down = lax.dot_general(tsum, diff * wcol, (((0,), (0,)), ((), ())), precision=lax.Precision.HIGHEST,
                           preferred_element_type=F32)
    down_ref[...] = down[:160]

    stage3(NBLK - 1)
    finish(NBLK - 2)
    finish(NBLK - 1)

    x_pair.wait_send()
    lab_pair.wait_send()
    st_pair.wait_send()
    for m in range(1, NUM_CHIPS):
        m_copy(m).wait_send()
    for i in range(NUM_CHIPS):
        @pl.when(core * 16 + i != me)
        def _():
            t_copy(i, chip).wait_send()

    def drain(j, carry):
        copy1(j).wait_send()
        copy2(j).wait_send()
        for m in (1, 2, 3):
            copy3(j, m).wait_send()
        out_local(j).wait()
        out_pair(j).wait()
        return carry

    lax.fori_loop(0, NBLK, drain, 0)


def solution(mesh):
    def local_step(tok_rows, w_up, w_down, heads, label_rows):
        hc = jnp.transpose(heads, (2, 0, 1)).reshape(2 * NUM_TASKS, DIM)
        vmem = pl.BlockSpec(memory_space=pltpu.VMEM)
        hbm = pl.BlockSpec(memory_space=pl.ANY)
        sds = jax.ShapeDtypeStruct
        dma = pltpu.SemaphoreType.DMA
        outs = pl.pallas_call(
            kernel,
            out_shape=(
                sds((NUM_TASKS, 128), F32),
                sds((40, HID), F32),
                sds((160, DIM), F32),
                sds((NBLK, NTB, TB, CW), BF16),
                sds((TOK, DIM), BF16),
            ),
            in_specs=[hbm, hbm, hbm, vmem, vmem],
            out_specs=(vmem, hbm, vmem, hbm, hbm),
            scratch_shapes=[
                pltpu.VMEM((5, TB, DIM), BF16),
                pltpu.VMEM((DIM, HALF), BF16),
                pltpu.VMEM((2, 2, 4 * ROWS, PAIR_TOK), BF16),
                pltpu.VMEM((24, TB, CW), BF16),
                pltpu.VMEM((HALF, 128), BF16),
                pltpu.VMEM((NUM_TASKS, HALF), F32),
                pltpu.VMEM((128, HALF), BF16),
                pltpu.VMEM((DIM, 128), BF16),
                pltpu.VMEM((NUM_TASKS, PAIR_TOK), F32),
                pltpu.VMEM((NUM_TASKS, PAIR_TOK), F32),
                pltpu.VMEM((NUM_TASKS, TOK), jnp.int32),
                pltpu.VMEM((PAIR_TOK, 128), BF16),
                pltpu.VMEM((32, PAIR_TOK), BF16),
                pltpu.VMEM((NUM_TASKS, HALF), F32),
                pltpu.VMEM((NUM_CHIPS, NUM_TASKS, 256), F32),
                pltpu.VMEM((NUM_CHIPS, NUM_TASKS, 256), F32),
                pltpu.VMEM((NUM_CHIPS, NUM_TASKS, 128), F32),
                pltpu.VMEM((NBLK, 2, 2, 4, ROWS, CW), F32),
                pltpu.VMEM((NBLK, 2, 4, ROWS, CW), F32),
                pltpu.VMEM((NBLK, 4, ROWS, CW), F32),
                pltpu.VMEM((NBLK, 3, ROWS, CW), F32),
                pltpu.VMEM((NBLK, 2, ROWS // 2, CW), F32),
                dma((5,)), dma((5,)), dma((5,)), dma((2, NBLK)), dma((2,)),
                dma((3,)), dma((3,)), dma((15,)), dma((15,)), dma((16,)), dma((16,)),
                dma((NBLK,)), dma((NBLK,)), dma((NBLK,)), dma((NBLK,)), dma((NBLK, 3)), dma((NBLK, 3)),
                dma((NBLK,)), dma((NBLK,)), dma((NBLK,)),
            ],
            compiler_params=pltpu.CompilerParams(
                collective_id=0, has_side_effects=True, vmem_limit_bytes=67043328),
        )(tok_rows, w_up, w_down, hc, label_rows)
        return outs[0][:, 0], outs[1], outs[2]

    return jax.shard_map(
        local_step, mesh=mesh, in_specs=(P('data', None), P(), P(), P(), P(None, 'data')),
        out_specs=(P(), P('data', None), P('data', None)), check_vma=False)
```

```python
import functools
import math

import jax
import jax.numpy as jnp
from jax import lax
from jax.experimental import pallas as pl
from jax.experimental.pallas import tpu as pltpu
from jax.sharding import PartitionSpec as P

F32 = jnp.float32
BF16 = jnp.bfloat16
MESH = pl.DeviceIdType.MESH
SOLVER_STEPS = 20
NUM_TASKS = 8
NUM_DEV = 32
NUM_CHIPS = 16
TOK = 2048
PAIR_TOK = 4096
DIM = 1280
HID = 5120
HALF = 2560
TB = 512
NTB = PAIR_TOK // TB
CW = 256
NBLK = HALF // CW
UW = 128
NUNIT = HALF // UW
LAGS = (1, 3, 4, 6)
ROWS = 80
C0 = math.sqrt(2.0 / math.pi)
C1 = C0 * 0.044715


def split3(v):
    hi = v.astype(BF16)
    rem = v - hi.astype(F32)
    mid = rem.astype(BF16)
    lo = (rem - mid.astype(F32)).astype(BF16)
    return hi, mid, lo


def dot(a, b, dims=((1,), (0,))):
    return lax.dot_general(a, b, (dims, ((), ())), preferred_element_type=F32)


def remote(src, dst, ssem, rsem, dev):
    return pltpu.make_async_remote_copy(
        src_ref=src, dst_ref=dst, send_sem=ssem, recv_sem=rsem,
        device_id=(dev,), device_id_type=MESH)


def sublane_sum(v):
    for sh in (4, 2, 1):
        v = v + pltpu.roll(v, sh, 0)
    return v


def rolled(v, k):
    return v if k == 0 else pltpu.roll(v, NUM_TASKS - k, 0)


def kernel(x_hbm, w1_hbm, w2_hbm, hc_ref, lab_ref,
           mix_ref, up_hbm, down_ref, a_hbm, xs_hbm,
           wbuf, w1, xt, abuf, gs, gt, agt, dpc, st, st_in, lab_in, rs, r3, tref, tp, trecv, mrecv,
           gbuf, q1, q2, q3, q4, fin,
           wsem, w1sem, xsem, asem, ainsem, pair_s, pair_r, msend, mrec, tsend, trec,
           rsend, rrecv, fs_loc, fs, fv):
    me = lax.axis_index("data")
    core = lax.rem(me, 2)
    chip = me // 2
    cx = lax.rem(chip, 2)
    cy = lax.rem(chip // 2, 2)
    cz = chip // 4
    sib = me + 1 - 2 * core

    def w2_load(c):
        return pltpu.make_async_copy(w2_hbm.at[pl.ds(pl.multiple_of(core * HALF + c * TB, TB), TB)], wbuf.at[c], wsem.at[c])

    def w1_load(c):
        return pltpu.make_async_copy(
            w1_hbm.at[:, pl.ds(pl.multiple_of(core * HALF + c * TB, TB), TB)], w1.at[:, pl.ds(c * TB, TB)], w1sem.at[c])

    def x_load_own(i, slot):
        return pltpu.make_async_copy(x_hbm.at[pl.ds(pl.multiple_of(i * TB, TB), TB)], wbuf.at[slot], xsem.at[slot])

    def x_load_sib(i, slot):
        return pltpu.make_async_copy(xs_hbm.at[pl.ds(pl.multiple_of((i - 4) * TB, TB), TB)], wbuf.at[slot], xsem.at[slot])

    for c in range(5):
        w2_load(c).start()
    for c in range(5):
        w1_load(c).start()

    barrier = pltpu.get_barrier_semaphore()
    for m in range(1, NUM_DEV):
        pl.semaphore_signal(barrier, inc=1, device_id=(lax.rem(me + m, NUM_DEV),), device_id_type=MESH)

    hc = hc_ref[...]
    diff = hc[:NUM_TASKS].astype(F32) - hc[NUM_TASKS:].astype(F32)
    dpieces = jnp.concatenate([p.astype(F32) for p in split3(diff)] + [jnp.zeros((104, DIM), F32)], axis=0)
    dpc[...] = dpieces.T.astype(BF16)
    for c in range(5):
        w2_load(c).wait()
        g24 = dot(wbuf[c], dpc[...])
        if c < 4:
            x_load_own(c, c).start()
        g24t = g24.T
        g8 = g24t[0:8] + g24t[8:16] + g24t[16:24]
        gt[:, c * TB:(c + 1) * TB] = g8
        pieces = jnp.concatenate([p.astype(F32) for p in split3(g8)] + [jnp.zeros((104, TB), F32)], axis=0)
        gs[c * TB:(c + 1) * TB, :] = pieces.T.astype(BF16)

    pl.semaphore_wait(barrier, NUM_DEV - 1)
    x_pair = remote(x_hbm, xs_hbm, pair_s.at[0], pair_r.at[0], sib)
    x_pair.start()
    lab_pair = remote(lab_ref, lab_in, pair_s.at[1], pair_r.at[1], sib)
    lab_pair.start()
    for c in range(5):
        w1_load(c).wait()

    def a_store(par, nb, at):
        return pltpu.make_async_copy(abuf.at[par * NBLK + nb], a_hbm.at[nb, at], asem.at[par, nb])

    def fwd(i, carry):
        slot = lax.rem(i, 5)
        par = lax.rem(i, 2)
        at = lax.rem(core * 4 + i, 8)
        col = pl.multiple_of(at * TB, TB)

        @pl.when(i == 3)
        def _():
            x_pair.wait_recv()

        @pl.when((i >= 3) & (i < 7))
        def _():
            x_load_sib(i + 1, lax.rem(i + 1, 5)).start()

        x_load_own(0, slot).wait()

        @pl.when(i >= 2)
        def _():
            for nb in range(NBLK):
                a_store(par, nb, at).wait()

        xb = wbuf[slot]
        total = None
        for t in range(5):
            pre = dot(xb, w1[:, t * TB:(t + 1) * TB]).astype(BF16)
            abuf[par * NBLK + 2 * t] = pre[:, :CW]
            abuf[par * NBLK + 2 * t + 1] = pre[:, CW:]
            af = pre.astype(F32)
            th = jnp.tanh(af * (C0 + C1 * (af * af)))
            h = 0.5 * af
            pb = (h + h * th).astype(BF16)
            part = dot(pb, gs[t * TB:(t + 1) * TB, :])
            total = part if total is None else total + part
        for nb in range(NBLK):
            a_store(par, nb, at).start()
        xbt = xb.T
        for c in range(NUM_CHIPS):
            zz, yy, xx = c // 4, (c // 2) % 2, c % 2
            row = (yy * 2 + zz // 2) * ROWS
            xt[zz % 2, xx, row:row + ROWS, pl.ds(col, TB)] = xbt[c * ROWS:(c + 1) * ROWS]
        tt = total.T
        st[:, pl.ds(col, TB)] = tt[0:8] + tt[8:16] + tt[16:24]

        @pl.when(i < 4)
        def _():
            xd = dot(wbuf[slot], dpc[...]).T
            st[:, pl.ds(col, TB)] += xd[0:8] + xd[8:16] + xd[16:24]

        return carry

    lax.fori_loop(0, NTB, fwd, 0)
    for par in range(2):
        for nb in range(NBLK):
            a_store(par, nb, 0).wait()

    st_pair = remote(st, st_in, pair_s.at[2], pair_r.at[2], sib)
    st_pair.start()

    def a_load(j):
        return pltpu.make_async_copy(
            a_hbm.at[j], abuf.at[pl.ds(pl.multiple_of(lax.rem(j, 2) * 8, 8), 8)], ainsem.at[lax.rem(j, 2)])

    a_load(0).start()
    lane = lax.broadcasted_iota(jnp.int32, (NUM_TASKS, 128), 1)
    dgram = jnp.zeros((NUM_TASKS, 128), F32)
    for k in range(NUM_TASKS):
        dgram = jnp.where(lane == k, jnp.sum(diff * rolled(diff, k), axis=1, keepdims=True), dgram)
    lab_pair.wait_recv()
    st_pair.wait_recv()
    own_col = pl.multiple_of(core * TOK, TOK)
    sib_col = pl.multiple_of((1 - core) * TOK, TOK)

    def resid(col, labels):
        delta = st[:, pl.ds(col, TOK)] + st_in[:, pl.ds(col, TOK)]
        sign = jnp.where(labels == 0, -1.0, 1.0)
        u = sign * delta
        e = jnp.exp(-jnp.abs(u))
        return sign * (jnp.where(u >= 0, 1.0, e) / (1.0 + e)) * (1.0 / (TOK * NUM_DEV))

    ra = resid(own_col, lab_ref[...])
    rb = resid(sib_col, lab_in[...])
    first = core == 0
    rlo = jnp.where(first, ra, rb)
    rhi = jnp.where(first, rb, ra)
    cg = jnp.zeros((NUM_TASKS, 128), F32)
    for k in range(NUM_TASKS):
        prod = rlo * rolled(rlo, k) + rhi * rolled(rhi, k)
        cg = jnp.where(lane == k, jnp.sum(prod, axis=1, keepdims=True), cg)
    mrecv[chip] = cg

    def m_copy(m):
        dst = lax.rem(chip + m, NUM_CHIPS) * 2 + core
        return remote(mrecv.at[chip], mrecv.at[chip], msend.at[m - 1], mrec.at[m - 1], dst)

    for m in range(1, NUM_CHIPS):
        m_copy(m).start()

    for part, r in ((0, rlo), (1, rhi)):
        hi, mid, lo = split3(r)
        base = part * TOK
        r3[:, base:base + TOK] = jnp.concatenate([hi.astype(F32), mid.astype(F32), lo.astype(F32), jnp.zeros_like(r)], axis=0).astype(BF16)
        hf, mf, lf = hi.astype(F32), mid.astype(F32), lo.astype(F32)
        for c in range(TOK // TB):
            sl = slice(c * TB, (c + 1) * TB)
            stack = jnp.concatenate([hf[:, sl], hf[:, sl], mf[:, sl], hf[:, sl], lf[:, sl], mf[:, sl], jnp.zeros((80, TB), F32)], axis=0)
            rs[base + c * TB:base + (c + 1) * TB, :] = stack.T.astype(BF16)

    for m in range(1, NUM_CHIPS):
        m_copy(m).wait_recv()
    mp = mrecv[0]
    for c in range(1, NUM_CHIPS):
        mp = mp + mrecv[c]
    mp = mp * dgram
    cols = [jnp.broadcast_to(mp[:, k:k + 1], (NUM_TASKS, 128)) for k in range(NUM_TASKS)]
    inv_scale = NUM_TASKS / sublane_sum(cols[0])

    def solve(step, w):
        ws = [rolled(w, k) for k in range(NUM_TASKS)]
        prods = [cols[k] * ws[k] for k in range(NUM_TASKS)]
        while len(ws) > 1:
            ws = [ws[i] + ws[i + 1] for i in range(0, len(ws), 2)]
            prods = [prods[i] + prods[i + 1] for i in range(0, len(prods), 2)]
        inv = 1.0 / ws[0]
        return (w * inv) * jnp.exp(-(prods[0] * inv) * inv_scale)

    wts = lax.fori_loop(0, SOLVER_STEPS, solve, jnp.full((NUM_TASKS, 128), 1.0 / NUM_TASKS, F32))
    wts = wts / sublane_sum(wts)
    mix_ref[...] = wts
    wcol = wts[:, 0:1]
    hi, mid, lo = [p.astype(F32) for p in split3(gt[...] * wcol)]
    agt[...] = jnp.concatenate([hi, mid, hi, lo, hi, mid, jnp.zeros((80, HALF), F32)], axis=0).astype(BF16)

    zl = lax.rem(cz, 2)
    zh = cz // 2
    to_x = me + 2 * (1 - 2 * cx)
    to_y = me + 4 * (1 - 2 * cy)
    to_zl = me + 8 * (1 - 2 * zl)
    to_zh = me + 16 * (1 - 2 * zh)
    pos1, pos2 = (cx, cy), (cy, cx)
    dev1, dev3 = (to_x, to_y), (to_y, to_x)

    def copy(j, h, s):
        u = 2 * j + h
        p1, p2 = pos1[h], pos2[h]
        if s == 1:
            src, dst, dev = gbuf.at[u, 1 - p1], q1.at[u], dev1[h]
        elif s == 2:
            src, dst, dev = gbuf.at[u, p1, 1 - zl], q2.at[u], to_zl
        elif s == 3:
            src, dst, dev = gbuf.at[u, p1, zl, 1 - p2], q3.at[u], dev3[h]
        else:
            src, dst, dev = gbuf.at[u, p1, zl, p2, 1 - zh], q4.at[u], to_zh
        return remote(src, dst, rsend.at[s - 1, u], rrecv.at[s - 1, u], dev)

    def out_cols(u):
        return pl.ds(pl.multiple_of(core * HALF + u * UW, UW), UW)

    def out_local(u):
        return pltpu.make_async_copy(fin.at[u, core], up_hbm.at[:, out_cols(u)], fs_loc.at[u])

    def out_pair(u):
        return remote(fin.at[u, 1 - core], up_hbm.at[:, out_cols(u)], fs.at[u], fv.at[u], sib)

    def stage(j, s):
        for h in range(2):
            u = 2 * j + h
            p1, p2 = pos1[h], pos2[h]
            copy(j, h, s - 1).wait_recv()
            if s == 2:
                gbuf[u, p1, 1 - zl] += q1[u, 1 - zl]
                copy(j, h, 2).start()
                gbuf[u, p1, zl] += q1[u, zl]
            elif s == 3:
                gbuf[u, p1, zl, 1 - p2] += q2[u, 1 - p2]
                copy(j, h, 3).start()
                gbuf[u, p1, zl, p2] += q2[u, p2]
            elif s == 4:
                gbuf[u, p1, zl, p2, 1 - zh] += q3[u, 1 - zh]
                copy(j, h, 4).start()
                gbuf[u, p1, zl, p2, zh] += q3[u, zh]
            else:
                tot = gbuf[u, p1, zl, p2, zh] + q4[u]
                fin[u, 0] = tot[:ROWS // 2]
                fin[u, 1] = tot[ROWS // 2:]
                out_local(u).start()
                out_pair(u).start()

    def block(j, carry):
        a_load(j).wait()

        @pl.when(j < NBLK - 1)
        def _():
            a_load(j + 1).start()

        jcol = pl.multiple_of(j * CW, CW)
        base = lax.rem(j, 2) * 8

        def elem(tb, tacc):
            row = pl.multiple_of(tb * TB, TB)
            af = abuf[base + tb].astype(F32)
            dp = dot(rs[pl.ds(row, TB), :], agt[:, pl.ds(jcol, CW)])
            a2 = af * af
            th = jnp.tanh(af * (C0 + C1 * a2))
            h = 0.5 * af
            pb = (h + h * th).astype(BF16)
            slope = (0.5 + 0.5 * th) + (h * (1.0 - th * th)) * (C0 + (3.0 * C1) * a2)
            abuf[16 + tb] = (dp * slope).astype(BF16)
            return tacc + dot(r3[:, pl.ds(row, TB)], pb)

        tacc = lax.fori_loop(0, NTB, elem, jnp.zeros((32, CW), F32))
        tref[:, pl.ds(jcol, CW)] = tacc[0:8] + tacc[8:16] + tacc[16:24]

        def chunk(q, c2):
            far = 1 - q // 2
            xi = far * (1 - cx) + (1 - far) * cx
            zi = lax.rem(q, 2)
            g = dot(xt[zi, xi], abuf[16:24].reshape(PAIR_TOK, CW)).reshape(2, 2, ROWS, CW)
            gbuf[2 * j, xi, zi] = g[:, :, :, :UW]
            for yi in range(2):
                gbuf[2 * j + 1, yi, zi, xi] = g[yi, :, :, UW:]

            @pl.when(q == 1)
            def _():
                copy(j, 0, 1).start()

            return c2

        lax.fori_loop(0, 4, chunk, 0)
        copy(j, 1, 1).start()
        for s, lag in zip((2, 3, 4, 5), LAGS):
            @pl.when(j >= lag)
            def _():
                stage(j - lag, s)

        return carry

    lax.fori_loop(0, NBLK, block, 0)

    for i in range(NUM_CHIPS):
        tp[i, :, 0:160] = tref[:, i * 160:(i + 1) * 160]

    def t_copy(i, src_chip):
        return remote(tp.at[i], trecv.at[src_chip], tsend.at[i], trec.at[src_chip], core * 16 + i)

    for i in range(NUM_CHIPS):
        @pl.when(core * 16 + i != me)
        def _():
            t_copy(i, chip).start()

        @pl.when(core * 16 + i == me)
        def _():
            trecv[chip] = tp[i]

    def late(b):
        for s, lag in zip((2, 3, 4, 5), LAGS):
            if b - lag < NBLK:
                stage(b - lag, s)

    late(NBLK)
    late(NBLK + 1)

    for c in range(NUM_CHIPS):
        @pl.when(c * 2 + me // 16 != me)
        def _():
            t_copy(0, c).wait_recv()

    tsum = trecv[0]
    for c in range(1, NUM_CHIPS):
        tsum = tsum + trecv[c]
    down = lax.dot_general(tsum, diff * wcol, (((0,), (0,)), ((), ())), precision=lax.Precision.HIGHEST,
                           preferred_element_type=F32)
    down_ref[...] = down[:160]

    for b in range(NBLK + 2, NBLK + LAGS[3]):
        late(b)

    x_pair.wait_send()
    lab_pair.wait_send()
    st_pair.wait_send()
    for m in range(1, NUM_CHIPS):
        m_copy(m).wait_send()
    for i in range(NUM_CHIPS):
        @pl.when(core * 16 + i != me)
        def _():
            t_copy(i, chip).wait_send()

    def drain(j, carry):
        for h in range(2):
            for s in range(1, 5):
                copy(j, h, s).wait_send()
            out_local(2 * j + h).wait()
            out_pair(2 * j + h).wait()
        return carry

    lax.fori_loop(0, NBLK, drain, 0)


def place(mix_in, up_in, down_in, mix_ref, up_hbm, down_hbm, ubuf, dbuf, sem):
    loads, stores = [], []
    for c in range(4):
        cu, cd = pl.ds(c * 1280, 1280), pl.ds(c * 40, 40)
        loads.append((pltpu.make_async_copy(up_in.at[:, cu], ubuf.at[:, cu], sem.at[0, c]),
                      pltpu.make_async_copy(down_in.at[cd], dbuf.at[cd], sem.at[1, c])))
        stores.append((pltpu.make_async_copy(ubuf.at[:, cu], up_hbm.at[:, cu], sem.at[2, c]),
                       pltpu.make_async_copy(dbuf.at[cd], down_hbm.at[cd], sem.at[3, c])))
    for pair in loads:
        for cp in pair:
            cp.start()
    w = mix_in[...]
    diag = lax.broadcasted_iota(jnp.int32, w.shape, 0) == lax.broadcasted_iota(jnp.int32, w.shape, 1)
    mix_ref[...] = jnp.sum(jnp.where(diag, w, 0.0), axis=0)[:NUM_TASKS]
    for ld, stp in zip(loads, stores):
        for a, b in zip(ld, stp):
            a.wait()
            b.start()
    for pair in stores:
        for cp in pair:
            cp.wait()


def solution(mesh):
    def local_step(tok_rows, w_up, w_down, heads, label_rows):
        hc = jnp.transpose(heads, (2, 0, 1)).reshape(2 * NUM_TASKS, DIM)
        vmem = pl.BlockSpec(memory_space=pltpu.VMEM)
        hbm = pl.BlockSpec(memory_space=pl.ANY)
        sds = jax.ShapeDtypeStruct
        dma = pltpu.SemaphoreType.DMA
        outs = pl.pallas_call(
            kernel,
            out_shape=(
                sds((NUM_TASKS, 128), F32),
                sds((40, HID), F32),
                sds((160, DIM), F32),
                sds((NBLK, NTB, TB, CW), BF16),
                sds((TOK, DIM), BF16),
            ),
            in_specs=[hbm, hbm, hbm, vmem, vmem],
            out_specs=(vmem, hbm, vmem, hbm, hbm),
            scratch_shapes=[
                pltpu.VMEM((5, TB, DIM), BF16),
                pltpu.VMEM((DIM, HALF), BF16),
                pltpu.VMEM((2, 2, 4 * ROWS, PAIR_TOK), BF16),
                pltpu.VMEM((24, TB, CW), BF16),
                pltpu.VMEM((HALF, 128), BF16),
                pltpu.VMEM((NUM_TASKS, HALF), F32),
                pltpu.VMEM((128, HALF), BF16),
                pltpu.VMEM((DIM, 128), BF16),
                pltpu.VMEM((NUM_TASKS, PAIR_TOK), F32),
                pltpu.VMEM((NUM_TASKS, PAIR_TOK), F32),
                pltpu.VMEM((NUM_TASKS, TOK), jnp.int32),
                pltpu.VMEM((PAIR_TOK, 128), BF16),
                pltpu.VMEM((32, PAIR_TOK), BF16),
                pltpu.VMEM((NUM_TASKS, HALF), F32),
                pltpu.VMEM((NUM_CHIPS, NUM_TASKS, 256), F32),
                pltpu.VMEM((NUM_CHIPS, NUM_TASKS, 256), F32),
                pltpu.VMEM((NUM_CHIPS, NUM_TASKS, 128), F32),
                pltpu.VMEM((NUNIT, 2, 2, 2, 2, ROWS, UW), F32),
                pltpu.VMEM((NUNIT, 2, 2, 2, ROWS, UW), F32),
                pltpu.VMEM((NUNIT, 2, 2, ROWS, UW), F32),
                pltpu.VMEM((NUNIT, 2, ROWS, UW), F32),
                pltpu.VMEM((NUNIT, ROWS, UW), F32),
                pltpu.VMEM((NUNIT, 2, ROWS // 2, UW), F32),
                dma((5,)), dma((5,)), dma((5,)), dma((2, NBLK)), dma((2,)),
                dma((3,)), dma((3,)), dma((15,)), dma((15,)), dma((16,)), dma((16,)),
                dma((4, NUNIT)), dma((4, NUNIT)), dma((NUNIT,)), dma((NUNIT,)), dma((NUNIT,)),
            ],
            compiler_params=pltpu.CompilerParams(
                collective_id=0, has_side_effects=True, vmem_limit_bytes=67043328),
        )(tok_rows, w_up, w_down, hc, label_rows)
        return pl.pallas_call(
            place,
            out_shape=(sds((NUM_TASKS,), F32), sds((40, HID), F32), sds((160, DIM), F32)),
            in_specs=[vmem, hbm, hbm],
            out_specs=(vmem, hbm, hbm),
            scratch_shapes=[pltpu.VMEM((40, HID), F32), pltpu.VMEM((160, DIM), F32), dma((4, 4))],
        )(*outs[:3])

    return jax.shard_map(
        local_step, mesh=mesh, in_specs=(P('data', None), P(), P(), P(), P(None, 'data')),
        out_specs=(P(), P('data', None), P('data', None)), check_vma=False)
```

```python
import functools
import math

import jax
import jax.numpy as jnp
from jax import lax
from jax.experimental import pallas as pl
from jax.experimental.pallas import tpu as pltpu
from jax.sharding import PartitionSpec as P

F32 = jnp.float32
BF16 = jnp.bfloat16
MESH = pl.DeviceIdType.MESH
SOLVER_STEPS = 20
NUM_TASKS = 8
NUM_DEV = 32
NUM_CHIPS = 16
TOK = 2048
PAIR_TOK = 4096
DIM = 1280
HID = 5120
HALF = 2560
TB = 512
NTB = PAIR_TOK // TB
CW = 256
NBLK = HALF // CW
UW = 128
NUNIT = HALF // UW
PLAN = ((0, 2, 1), (1, 3, 3), (1, 4, 4), (2, 5, 6))
ROWS = 80
C0 = math.sqrt(2.0 / math.pi)
C1 = C0 * 0.044715


def split3(v):
    hi = v.astype(BF16)
    rem = v - hi.astype(F32)
    mid = rem.astype(BF16)
    lo = (rem - mid.astype(F32)).astype(BF16)
    return hi, mid, lo


def dot(a, b, dims=((1,), (0,))):
    return lax.dot_general(a, b, (dims, ((), ())), preferred_element_type=F32)


def remote(src, dst, ssem, rsem, dev):
    return pltpu.make_async_remote_copy(
        src_ref=src, dst_ref=dst, send_sem=ssem, recv_sem=rsem,
        device_id=(dev,), device_id_type=MESH)


def sublane_sum(v):
    for sh in (4, 2, 1):
        v = v + pltpu.roll(v, sh, 0)
    return v


def rolled(v, k):
    return v if k == 0 else pltpu.roll(v, NUM_TASKS - k, 0)


def kernel(x_hbm, w1_hbm, w2_hbm, hc_ref, lab_ref,
           mix_ref, up_hbm, tsum_ref, ad_ref, a_hbm, xs_hbm,
           wbuf, w1, xt, abuf, da0, da1, pref, stx, gs, gt, dpc, st, st_in, lab_in, r3, tref, tp, trecv, mrecv,
           gbuf, q1, q2, q3, q4,
           w2sem, w1sem, xsem, asem, ainsem, pair_s, pair_r, msend, mrec, tsend, trec,
           rsend, rrecv, fs_loc, fs, fv):
    me = lax.axis_index("data")
    core = lax.rem(me, 2)
    chip = me // 2
    cx = lax.rem(chip, 2)
    cy = lax.rem(chip // 2, 2)
    cz = chip // 4
    sib = me + 1 - 2 * core

    def w2_tile(n):
        return da0.at[n] if n < 8 else da1.at[n - 8] if n < 16 else abuf.at[n - 6]

    def w2_load(n):
        rows = pl.ds(pl.multiple_of(core * HALF + n // 5 * TB, TB), TB)
        return pltpu.make_async_copy(w2_hbm.at[rows, pl.ds(n % 5 * CW, CW)], w2_tile(n), w2sem.at[n])

    def w1_load(c):
        return pltpu.make_async_copy(
            w1_hbm.at[:, pl.ds(pl.multiple_of(core * HALF + c * TB, TB), TB)], w1.at[:, pl.ds(c * TB, TB)], w1sem.at[c])

    def x_load_own(i):
        return pltpu.make_async_copy(x_hbm.at[pl.ds(i * TB, TB)], wbuf.at[i], xsem.at[i])

    def x_load_sib(i, slot):
        return pltpu.make_async_copy(xs_hbm.at[pl.ds(pl.multiple_of((i - 4) * TB, TB), TB)], wbuf.at[slot], xsem.at[slot])

    x_load_own(0).start()
    for c in range(5):
        w1_load(c).start()
    for c in range(1, 4):
        x_load_own(c).start()
    for n in range(25):
        w2_load(n).start()

    barrier = pltpu.get_barrier_semaphore()
    for m in range(1, NUM_DEV):
        pl.semaphore_signal(barrier, inc=1, device_id=(lax.rem(me + m, NUM_DEV),), device_id_type=MESH)

    def fold(v):
        return v[0:8] + v[8:16] + v[16:24]

    def wide(parts, rows, cols):
        return jnp.concatenate([p.astype(F32) for p in parts] + [jnp.zeros((128 - rows, cols), F32)], axis=0)

    diff = hc_ref[:, 0, :].astype(F32) - hc_ref[:, 1, :].astype(F32)
    dpc[...] = wide(split3(diff), 24, DIM).T.astype(BF16)
    def a_store(par, nb, at):
        return pltpu.make_async_copy(abuf.at[par * NBLK + nb], a_hbm.at[nb, at], asem.at[par, nb])

    def gelu16(v):
        af = v.astype(F32)
        h = 0.5 * af
        return (h + h * jnp.tanh(af * (C0 + C1 * (af * af)))).astype(BF16)

    def block_col(i):
        return pl.multiple_of(lax.rem(core * 4 + i, 8) * TB, TB)

    def finish_prev(par, col):
        tot = dot(pref[...], gs[0:4 * TB, :])
        for n in (8, 9):
            tot = tot + dot(gelu16(abuf[par * NBLK + n]), gs[n * CW:(n + 1) * CW, :])
        st[:, pl.ds(col, TB)] = fold(tot.T)

    def fwd_block(i, first):
        slot = lax.rem(i, 4)
        par = lax.rem(i, 2)
        at = lax.rem(core * 4 + i, 8)
        col = block_col(i)

        if first:
            x_load_own(0).wait()
        else:
            @pl.when(i == 3)
            def _():
                x_pair.wait_recv()

            @pl.when((i >= 3) & (i < 7))
            def _():
                x_load_sib(i + 1, lax.rem(i + 1, 4)).start()

            @pl.when(i >= 4)
            def _():
                x_load_sib(i, slot).wait()

            @pl.when(i >= 2)
            def _():
                for nb in range(NBLK):
                    a_store(par, nb, at).wait()

        xb = wbuf[slot]

        def tile(t):
            if first:
                w1_load(t).wait()
            pre = dot(xb, w1[:, t * TB:(t + 1) * TB]).astype(BF16)
            abuf[par * NBLK + 2 * t] = pre[:, :CW]
            abuf[par * NBLK + 2 * t + 1] = pre[:, CW:]
            return pre

        pre = tile(0)
        if not first:
            finish_prev(1 - par, block_col(i + 7))
        pref[:, 0:TB] = gelu16(pre)
        for t in range(1, 4):
            pref[:, t * TB:(t + 1) * TB] = gelu16(tile(t))
        tile(4)
        xbt = xb.T
        for c in range(NUM_CHIPS):
            zz, yy, xx = c // 4, (c // 2) % 2, c % 2
            row = (yy * 2 + zz // 2) * ROWS
            xt[zz % 2, xx, row:row + ROWS, pl.ds(col, TB)] = xbt[c * ROWS:(c + 1) * ROWS]
        for nb in range(NBLK):
            a_store(par, nb, at).start()

    fwd_block(0, True)

    for c in range(1, 4):
        x_load_own(c).wait()
    for n in range(25):
        w2_load(n).wait()
    for c in range(4):
        stx[:, c * TB:(c + 1) * TB] = fold(dot(wbuf[c], dpc[...]).T)
    for c in range(5):
        g24 = dot(w2_tile(5 * c)[...], dpc[0:CW, :])
        for kc in range(1, 5):
            g24 = g24 + dot(w2_tile(5 * c + kc)[...], dpc[kc * CW:(kc + 1) * CW, :])
        g8 = fold(g24.T)
        gt[:, c * TB:(c + 1) * TB] = g8
        gs[c * TB:(c + 1) * TB, :] = wide(split3(g8), 24, TB).T.astype(BF16)

    pl.semaphore_wait(barrier, NUM_DEV - 1)
    x_pair = remote(x_hbm, xs_hbm, pair_s.at[0], pair_r.at[0], sib)
    x_pair.start()
    lab_pair = remote(lab_ref, lab_in, pair_s.at[1], pair_r.at[1], sib)
    lab_pair.start()

    def fwd(i, carry):
        fwd_block(i, False)
        return carry

    lax.fori_loop(1, NTB, fwd, 0)
    finish_prev(1, block_col(7))
    own = pl.ds(pl.multiple_of(core * TOK, TOK), TOK)
    st[:, own] += stx[...]
    for par in range(2):
        for nb in range(NBLK):
            a_store(par, nb, 0).wait()

    st_pair = remote(st, st_in, pair_s.at[2], pair_r.at[2], sib)
    st_pair.start()

    def a_load(j):
        return pltpu.make_async_copy(
            a_hbm.at[j], abuf.at[pl.ds(pl.multiple_of(lax.rem(j, 2) * 8, 8), 8)], ainsem.at[lax.rem(j, 2)])

    a_load(0).start()
    a_load(1).start()
    agt = w1.at[0:128]

    def resid_tile(tb):
        return wbuf.at[lax.rem(tb, 4), :, pl.ds(pl.multiple_of(tb // 4 * 128, 128), 128)]

    lane = lax.broadcasted_iota(jnp.int32, (NUM_TASKS, 128), 1)
    dgram = jnp.zeros((NUM_TASKS, 128), F32)
    for k in range(NUM_TASKS):
        dgram = jnp.where(lane == k, jnp.sum(diff * rolled(diff, k), axis=1, keepdims=True), dgram)
    lab_pair.wait_recv()
    st_pair.wait_recv()
    own_col = pl.multiple_of(core * TOK, TOK)
    sib_col = pl.multiple_of((1 - core) * TOK, TOK)

    def resid(col, labels):
        delta = st[:, pl.ds(col, TOK)] + st_in[:, pl.ds(col, TOK)]
        sign = jnp.where(labels == 0, -1.0, 1.0)
        u = sign * delta
        e = jnp.exp(-jnp.abs(u))
        return sign * (jnp.where(u >= 0, 1.0, e) / (1.0 + e)) * (1.0 / (TOK * NUM_DEV))

    ra = resid(own_col, lab_ref[...])
    rb = resid(sib_col, lab_in[...])
    first = core == 0
    rlo = jnp.where(first, ra, rb)
    rhi = jnp.where(first, rb, ra)
    cg = jnp.zeros((NUM_TASKS, 128), F32)
    for k in range(NUM_TASKS):
        prod = rlo * rolled(rlo, k) + rhi * rolled(rhi, k)
        cg = jnp.where(lane == k, jnp.sum(prod, axis=1, keepdims=True), cg)
    mrecv[chip] = cg

    def m_copy(m):
        dst = lax.rem(chip + m, NUM_CHIPS) * 2 + core
        return remote(mrecv.at[chip], mrecv.at[chip], msend.at[m - 1], mrec.at[m - 1], dst)

    for m in range(1, NUM_CHIPS):
        m_copy(m).start()

    for part, r in ((0, rlo), (1, rhi)):
        hi, mid, lo = split3(r)
        base = part * TOK
        r3[:, base:base + TOK] = jnp.concatenate([hi.astype(F32), mid.astype(F32), lo.astype(F32), jnp.zeros_like(r)], axis=0).astype(BF16)
        hf, mf, lf = hi.astype(F32), mid.astype(F32), lo.astype(F32)
        for c in range(TOK // TB):
            sl = slice(c * TB, (c + 1) * TB)
            stack = jnp.concatenate([hf[:, sl], hf[:, sl], mf[:, sl], hf[:, sl], lf[:, sl], mf[:, sl], jnp.zeros((80, TB), F32)], axis=0)
            wbuf[c, :, part * 128:(part + 1) * 128] = stack.T.astype(BF16)

    def slope_of(af):
        a2 = af * af
        th = jnp.tanh(af * (C0 + C1 * a2))
        h = 0.5 * af
        slope = (0.5 + 0.5 * th) + (h * (1.0 - th * th)) * (C0 + (3.0 * C1) * a2)
        return (h + h * th).astype(BF16), slope

    a_load(0).wait()

    def slope0(tb, tacc):
        pb, slope = slope_of(abuf[tb].astype(F32))
        for h in range(2):
            gbuf[12 + tb, h, :, :, :, 0:64] = slope[:, h * UW:(h + 1) * UW].reshape(2, 2, 2, 64, UW)
        return tacc + dot(r3[:, pl.ds(pl.multiple_of(tb * TB, TB), TB)], pb)

    tacc = lax.fori_loop(0, NTB, slope0, jnp.zeros((32, CW), F32))
    tref[:, 0:CW] = fold(tacc)

    for m in range(1, NUM_CHIPS):
        m_copy(m).wait_recv()
    mp = mrecv[0]
    for c in range(1, NUM_CHIPS):
        mp = mp + mrecv[c]
    mp = mp * dgram
    cols = [jnp.broadcast_to(mp[:, k:k + 1], (NUM_TASKS, 128)) for k in range(NUM_TASKS)]
    inv_scale = NUM_TASKS / sublane_sum(cols[0])

    def solve(step, w):
        ws = [rolled(w, k) for k in range(NUM_TASKS)]
        prods = [cols[k] * ws[k] for k in range(NUM_TASKS)]
        while len(ws) > 1:
            ws = [ws[i] + ws[i + 1] for i in range(0, len(ws), 2)]
            prods = [prods[i] + prods[i + 1] for i in range(0, len(prods), 2)]
        inv = 1.0 / ws[0]
        return (w * inv) * jnp.exp(-(prods[0] * inv) * inv_scale)

    wts = lax.fori_loop(0, SOLVER_STEPS, solve, jnp.full((NUM_TASKS, 128), 1.0 / NUM_TASKS, F32))
    wts = wts / sublane_sum(wts)
    mix_ref[...] = wts
    wcol = wts[:, 0:1]
    hi, mid, lo = [p.astype(F32) for p in split3(gt[...] * wcol)]
    agt[...] = jnp.concatenate([hi, mid, hi, lo, hi, mid, jnp.zeros((80, HALF), F32)], axis=0).astype(BF16)

    zl = lax.rem(cz, 2)
    zh = cz // 2
    to_x = me + 2 * (1 - 2 * cx)
    to_y = me + 4 * (1 - 2 * cy)
    to_zl = me + 8 * (1 - 2 * zl)
    to_zh = me + 16 * (1 - 2 * zh)
    pos1, pos2 = (cx, cy), (cy, cx)
    dev1, dev3 = (to_x, to_y), (to_y, to_x)

    def copy(j, h, s):
        u = 2 * j + h
        p1, p2 = pos1[h], pos2[h]
        if s < 2:
            zi = 1 - zl if s == 0 else zl
            src, dst, dev = gbuf.at[u, 1 - p1, zi], q1.at[u, zi], dev1[h]
        elif s == 2:
            src, dst, dev = gbuf.at[u, p1, 1 - zl], q2.at[u], to_zl
        elif s == 3:
            src, dst, dev = gbuf.at[u, p1, zl, 1 - p2], q3.at[u], dev3[h]
        else:
            src, dst, dev = gbuf.at[u, p1, zl, p2, 1 - zh], q4.at[u], to_zh
        return remote(src, dst, rsend.at[s, u], rrecv.at[s, u], dev)

    def out_cols(u):
        return pl.ds(pl.multiple_of(core * HALF + u * UW, UW), UW)

    def result(u, half):
        h = lax.rem(u, 2)
        p1 = (1 - h) * cx + h * cy
        p2 = (1 - h) * cy + h * cx
        return gbuf.at[u, p1, zl, p2, zh, pl.ds(pl.multiple_of(half * (ROWS // 2), 8), ROWS // 2)]

    def out_local(u):
        return pltpu.make_async_copy(result(u, core), up_hbm.at[:, out_cols(u)], fs_loc.at[u])

    def out_pair(u):
        return remote(result(u, 1 - core), up_hbm.at[:, out_cols(u)], fs.at[u], fv.at[u], sib)

    def stage(j, s):
        for h in range(2):
            u = 2 * j + h
            p1, p2 = pos1[h], pos2[h]
            if s == 2:
                copy(j, h, 0).wait_recv()
                gbuf[u, p1, 1 - zl] += q1[u, 1 - zl]
                copy(j, h, 2).start()
            elif s == 3:
                copy(j, h, 1).wait_recv()
                copy(j, h, 2).wait_recv()
                gbuf[u, p1, zl, 1 - p2] += q1[u, zl, 1 - p2] + q2[u, 1 - p2]
                copy(j, h, 3).start()
                gbuf[u, p1, zl, p2] += q1[u, zl, p2] + q2[u, p2]
            elif s == 4:
                copy(j, h, 3).wait_recv()
                gbuf[u, p1, zl, p2, 1 - zh] += q3[u, 1 - zh]
                copy(j, h, 4).start()
                gbuf[u, p1, zl, p2, zh] += q3[u, zh]
            else:
                copy(j, h, 4).wait_recv()
                gbuf[u, p1, zl, p2, zh] += q4[u]
                out_local(u).start()
                out_pair(u).start()

    def elem0(tb, carry):
        dp = dot(resid_tile(tb)[...], agt[:, 0:CW])
        for h in range(2):
            slope = gbuf[12 + tb, h, :, :, :, 0:64].reshape(TB, UW)
            da0[tb, :, h * UW:(h + 1) * UW] = (dp[:, h * UW:(h + 1) * UW] * slope).astype(BF16)
        return carry

    lax.fori_loop(0, NTB, elem0, 0)

    def block(j, cur, nxt):
        @pl.when(j < NBLK - 1)
        def _():
            a_load(j + 1).wait()

        @pl.when(j < NBLK - 2)
        def _():
            a_load(j + 2).start()

        ncol = pl.multiple_of(jnp.minimum(j + 1, NBLK - 1) * CW, CW)
        base = lax.rem(j + 1, 2) * 8

        def chunk(q, tacc):
            far = 1 - lax.rem(q, 2)
            xi = far * (1 - cx) + (1 - far) * cx
            near = q // 2
            zi = (1 - near) * (1 - zl) + near * zl
            g = dot(xt[zi, xi], cur[...].reshape(PAIR_TOK, CW)).reshape(2, 2, ROWS, CW)
            gbuf[2 * j, xi, zi] = g[:, :, :, :UW]
            for yi in range(2):
                gbuf[2 * j + 1, yi, zi, xi] = g[yi, :, :, UW:]
            for n in range(2):
                tb = 2 * q + n
                rows = pl.ds(pl.multiple_of(tb * TB, TB), TB)
                pb, slope = slope_of(abuf[base + tb].astype(F32))
                dp = dot(resid_tile(tb)[...], agt[:, pl.ds(ncol, CW)])
                nxt[tb] = (dp * slope).astype(BF16)
                tacc = tacc + dot(r3[:, rows], pb)

            for k, (h, part) in enumerate(((0, 0), (1, 0), (0, 1), (1, 1))):
                @pl.when(q == k)
                def _():
                    copy(j, h, part).start()

            for k, s, lag in PLAN:
                @pl.when((q == k) & (j >= lag))
                def _():
                    stage(j - lag, s)

            return tacc

        tacc = lax.fori_loop(0, 4, chunk, jnp.zeros((32, CW), F32))

        @pl.when(j < NBLK - 1)
        def _():
            tref[:, pl.ds(ncol, CW)] = fold(tacc)

    def two_blocks(jj, carry):
        block(2 * jj, da0, da1)
        block(2 * jj + 1, da1, da0)
        return carry

    lax.fori_loop(0, NBLK // 2, two_blocks, 0)

    for i in range(NUM_CHIPS):
        tp[i, :, 0:160] = tref[:, i * 160:(i + 1) * 160]

    def t_copy(i, src_chip):
        return remote(tp.at[i], trecv.at[src_chip], tsend.at[i], trec.at[src_chip], core * 16 + i)

    for i in range(NUM_CHIPS):
        @pl.when(core * 16 + i != me)
        def _():
            t_copy(i, chip).start()

        @pl.when(core * 16 + i == me)
        def _():
            trecv[chip] = tp[i]

    def late(b):
        for _, s, lag in PLAN:
            if b - lag < NBLK:
                stage(b - lag, s)

    late(NBLK)
    late(NBLK + 1)

    for c in range(NUM_CHIPS):
        @pl.when(c * 2 + me // 16 != me)
        def _():
            t_copy(0, c).wait_recv()

    tsum = trecv[0]
    for c in range(1, NUM_CHIPS):
        tsum = tsum + trecv[c]
    tsum_ref[...] = tsum
    ad_ref[...] = diff * wcol

    for b in range(NBLK + 2, NBLK + PLAN[-1][2]):
        late(b)

    x_pair.wait_send()
    lab_pair.wait_send()
    st_pair.wait_send()
    for m in range(1, NUM_CHIPS):
        m_copy(m).wait_send()
    for i in range(NUM_CHIPS):
        @pl.when(core * 16 + i != me)
        def _():
            t_copy(i, chip).wait_send()

    def drain(j, carry):
        for h in range(2):
            for s in range(5):
                copy(j, h, s).wait_send()
            out_local(2 * j + h).wait()
            out_pair(2 * j + h).wait()
        return carry

    lax.fori_loop(0, NBLK, drain, 0)


def place(mix_in, up_in, tsum_in, ad_in, mix_ref, up_hbm, down_hbm, ubuf, dbuf, sem):
    cols = [pl.ds(c * 1280, 1280) for c in range(4)]
    loads = [pltpu.make_async_copy(up_in.at[:, cu], ubuf.at[:, cu], sem.at[0, c]) for c, cu in enumerate(cols)]
    stores = [pltpu.make_async_copy(ubuf.at[:, cu], up_hbm.at[:, cu], sem.at[1, c]) for c, cu in enumerate(cols)]
    for cp in loads:
        cp.start()
    w = mix_in[...]
    diag = lax.broadcasted_iota(jnp.int32, w.shape, 0) == lax.broadcasted_iota(jnp.int32, w.shape, 1)
    mix_ref[...] = jnp.sum(jnp.where(diag, w, 0.0), axis=0)[:NUM_TASKS]
    down = lax.dot_general(tsum_in[...], ad_in[...], (((0,), (0,)), ((), ())), precision=lax.Precision.HIGHEST,
                           preferred_element_type=F32)
    dbuf[...] = down[:160]
    put = pltpu.make_async_copy(dbuf, down_hbm, sem.at[0, 4])
    put.start()
    for a, b in zip(loads, stores):
        a.wait()
        b.start()
    for cp in stores:
        cp.wait()
    put.wait()


def solution(mesh):
    def local_step(tok_rows, w_up, w_down, heads, label_rows):
        hc = jnp.transpose(heads, (0, 2, 1))
        vmem = pl.BlockSpec(memory_space=pltpu.VMEM)
        hbm = pl.BlockSpec(memory_space=pl.ANY)
        sds = jax.ShapeDtypeStruct
        dma = pltpu.SemaphoreType.DMA
        outs = pl.pallas_call(
            kernel,
            out_shape=(
                sds((NUM_TASKS, 128), F32),
                sds((40, HID), F32),
                sds((NUM_TASKS, 256), F32),
                sds((NUM_TASKS, DIM), F32),
                sds((NBLK, NTB, TB, CW), BF16),
                sds((TOK, DIM), BF16),
            ),
            in_specs=[hbm, hbm, hbm, vmem, vmem],
            out_specs=(vmem, hbm, vmem, vmem, hbm, hbm),
            scratch_shapes=[
                pltpu.VMEM((4, TB, DIM), BF16),
                pltpu.VMEM((DIM, HALF), BF16),
                pltpu.VMEM((2, 2, 4 * ROWS, PAIR_TOK), BF16),
                pltpu.VMEM((20, TB, CW), BF16),
                pltpu.VMEM((NTB, TB, CW), BF16),
                pltpu.VMEM((NTB, TB, CW), BF16),
                pltpu.VMEM((TB, 4 * TB), BF16),
                pltpu.VMEM((NUM_TASKS, TOK), F32),
                pltpu.VMEM((HALF, 128), BF16),
                pltpu.VMEM((NUM_TASKS, HALF), F32),
                pltpu.VMEM((DIM, 128), BF16),
                pltpu.VMEM((NUM_TASKS, PAIR_TOK), F32),
                pltpu.VMEM((NUM_TASKS, PAIR_TOK), F32),
                pltpu.VMEM((NUM_TASKS, TOK), jnp.int32),
                pltpu.VMEM((32, PAIR_TOK), BF16),
                pltpu.VMEM((NUM_TASKS, HALF), F32),
                pltpu.VMEM((NUM_CHIPS, NUM_TASKS, 256), F32),
                pltpu.VMEM((NUM_CHIPS, NUM_TASKS, 256), F32),
                pltpu.VMEM((NUM_CHIPS, NUM_TASKS, 128), F32),
                pltpu.VMEM((NUNIT, 2, 2, 2, 2, ROWS, UW), F32),
                pltpu.VMEM((NUNIT, 2, 2, 2, ROWS, UW), F32),
                pltpu.VMEM((NUNIT, 2, 2, ROWS, UW), F32),
                pltpu.VMEM((NUNIT, 2, ROWS, UW), F32),
                pltpu.VMEM((NUNIT, ROWS, UW), F32),
                dma((25,)), dma((5,)), dma((4,)), dma((2, NBLK)), dma((2,)),
                dma((3,)), dma((3,)), dma((15,)), dma((15,)), dma((16,)), dma((16,)),
                dma((5, NUNIT)), dma((5, NUNIT)), dma((NUNIT,)), dma((NUNIT,)), dma((NUNIT,)),
            ],
            compiler_params=pltpu.CompilerParams(
                collective_id=0, has_side_effects=True, vmem_limit_bytes=67043328),
        )(tok_rows, w_up, w_down, hc, label_rows)
        return pl.pallas_call(
            place,
            out_shape=(sds((NUM_TASKS,), F32), sds((40, HID), F32), sds((160, DIM), F32)),
            in_specs=[vmem, hbm, vmem, vmem],
            out_specs=(vmem, hbm, hbm),
            scratch_shapes=[pltpu.VMEM((40, HID), F32), pltpu.VMEM((160, DIM), F32), dma((2, 5))],
        )(*outs[:4])

    return jax.shard_map(
        local_step, mesh=mesh, in_specs=(P('data', None), P(), P(), P(), P(None, 'data')),
        out_specs=(P(), P('data', None), P('data', None)), check_vma=False)
```

```python
import functools
import math

import jax
import jax.numpy as jnp
from jax import lax
from jax.experimental import pallas as pl
from jax.experimental.pallas import tpu as pltpu
from jax.sharding import PartitionSpec as P

F32 = jnp.float32
BF16 = jnp.bfloat16
MESH = pl.DeviceIdType.MESH
SOLVER_STEPS = 20
NUM_TASKS = 8
NUM_DEV = 32
NUM_CHIPS = 16
TOK = 2048
PAIR_TOK = 4096
DIM = 1280
HID = 5120
HALF = 2560
TB = 512
NTB = PAIR_TOK // TB
CW = 256
NBLK = HALF // CW
UW = 128
NUNIT = HALF // UW
PLAN = ((0, 2, 1), (1, 3, 3), (1, 4, 4), (2, 5, 6))
ROWS = 80
C0 = math.sqrt(2.0 / math.pi)
C1 = C0 * 0.044715


def split3(v):
    hi = v.astype(BF16)
    rem = v - hi.astype(F32)
    mid = rem.astype(BF16)
    lo = (rem - mid.astype(F32)).astype(BF16)
    return hi, mid, lo


def dot(a, b, dims=((1,), (0,))):
    return lax.dot_general(a, b, (dims, ((), ())), preferred_element_type=F32)


def remote(src, dst, ssem, rsem, dev):
    return pltpu.make_async_remote_copy(
        src_ref=src, dst_ref=dst, send_sem=ssem, recv_sem=rsem,
        device_id=(dev,), device_id_type=MESH)


def sublane_sum(v):
    for sh in (4, 2, 1):
        v = v + pltpu.roll(v, sh, 0)
    return v


def rolled(v, k):
    return v if k == 0 else pltpu.roll(v, NUM_TASKS - k, 0)


def kernel(x_hbm, w1_hbm, w2_hbm, hc_ref, lab_ref,
           mix_ref, up_hbm, tsum_ref, ad_ref, a_hbm, xs_hbm,
           wbuf, w1, xt, abuf, da0, da1, pref, stx, gs, gt, dpc, st, st_in, lab_in, r3, tref, tp, trecv, mrecv,
           gbuf, q1, q2, q3, q4,
           w2sem, w1sem, xsem, asem, ainsem, pair_s, pair_r, msend, mrec, tsend, trec,
           rsend, rrecv, fs_loc, fs, fv):
    me = lax.axis_index("data")
    core = lax.rem(me, 2)
    chip = me // 2
    cx = lax.rem(chip, 2)
    cy = lax.rem(chip // 2, 2)
    cz = chip // 4
    sib = me + 1 - 2 * core

    def w2_tile(n):
        return da0.at[n] if n < 8 else da1.at[n - 8] if n < 16 else abuf.at[n - 6]

    def w2_load(n):
        rows = pl.ds(pl.multiple_of(core * HALF + n // 5 * TB, TB), TB)
        return pltpu.make_async_copy(w2_hbm.at[rows, pl.ds(n % 5 * CW, CW)], w2_tile(n), w2sem.at[n])

    def w1_load(c):
        return pltpu.make_async_copy(
            w1_hbm.at[:, pl.ds(pl.multiple_of(core * HALF + c * TB, TB), TB)], w1.at[:, pl.ds(c * TB, TB)], w1sem.at[c])

    def x_load_own(i):
        return pltpu.make_async_copy(x_hbm.at[pl.ds(i * TB, TB)], wbuf.at[i], xsem.at[i])

    def x_load_sib(i, slot):
        return pltpu.make_async_copy(xs_hbm.at[pl.ds(pl.multiple_of((i - 4) * TB, TB), TB)], wbuf.at[slot], xsem.at[slot])

    x_load_own(0).start()
    for c in range(5):
        w1_load(c).start()
    for c in range(1, 4):
        x_load_own(c).start()
    for n in range(25):
        w2_load(n).start()

    barrier = pltpu.get_barrier_semaphore()
    for m in range(1, NUM_DEV):
        pl.semaphore_signal(barrier, inc=1, device_id=(lax.rem(me + m, NUM_DEV),), device_id_type=MESH)

    def fold(v):
        return v[0:8] + v[8:16] + v[16:24]

    def wide(parts, rows, cols):
        return jnp.concatenate([p.astype(F32) for p in parts] + [jnp.zeros((128 - rows, cols), F32)], axis=0)

    diff = hc_ref[:, 0, :].astype(F32) - hc_ref[:, 1, :].astype(F32)
    dpc[...] = wide(split3(diff), 24, DIM).T.astype(BF16)
    def a_store(par, nb, at):
        return pltpu.make_async_copy(abuf.at[par * NBLK + nb], a_hbm.at[nb, at], asem.at[par, nb])

    def gelu16(v):
        af = v.astype(F32)
        h = 0.5 * af
        return (h + h * jnp.tanh(af * (C0 + C1 * (af * af)))).astype(BF16)

    def block_col(i):
        return pl.multiple_of(lax.rem(core * 4 + i, 8) * TB, TB)

    def finish_prev(par, col):
        tot = dot(pref[...], gs[0:4 * TB, :])
        for n in (8, 9):
            tot = tot + dot(gelu16(abuf[par * NBLK + n]), gs[n * CW:(n + 1) * CW, :])
        st[:, pl.ds(col, TB)] = fold(tot.T)

    def fwd_block(i, first):
        slot = lax.rem(i, 4)
        par = lax.rem(i, 2)
        at = lax.rem(core * 4 + i, 8)
        col = block_col(i)

        if first:
            x_load_own(0).wait()
        else:
            @pl.when(i == 3)
            def _():
                x_pair.wait_recv()

            @pl.when((i >= 3) & (i < 7))
            def _():
                x_load_sib(i + 1, lax.rem(i + 1, 4)).start()

            @pl.when(i >= 4)
            def _():
                x_load_sib(i, slot).wait()

            @pl.when(i >= 2)
            def _():
                for nb in range(NBLK):
                    a_store(par, nb, at).wait()

        xb = wbuf[slot]

        def tile(t):
            if first:
                w1_load(t).wait()
            pre = dot(xb, w1[:, t * TB:(t + 1) * TB]).astype(BF16)
            abuf[par * NBLK + 2 * t] = pre[:, :CW]
            abuf[par * NBLK + 2 * t + 1] = pre[:, CW:]
            return pre

        pre = tile(0)
        if not first:
            finish_prev(1 - par, block_col(i + 7))
        pref[:, 0:TB] = gelu16(pre)
        for t in range(1, 4):
            pref[:, t * TB:(t + 1) * TB] = gelu16(tile(t))
        tile(4)
        xbt = xb.T
        for c in range(NUM_CHIPS):
            zz, yy, xx = c // 4, (c // 2) % 2, c % 2
            row = (yy * 2 + zz // 2) * ROWS
            xt[zz % 2, xx, row:row + ROWS, pl.ds(col, TB)] = xbt[c * ROWS:(c + 1) * ROWS]
        for nb in range(NBLK):
            a_store(par, nb, at).start()

    fwd_block(0, True)

    for c in range(1, 4):
        x_load_own(c).wait()
    for n in range(25):
        w2_load(n).wait()
    for c in range(4):
        stx[:, c * TB:(c + 1) * TB] = fold(dot(wbuf[c], dpc[...]).T)
    for c in range(5):
        g24 = dot(w2_tile(5 * c)[...], dpc[0:CW, :])
        for kc in range(1, 5):
            g24 = g24 + dot(w2_tile(5 * c + kc)[...], dpc[kc * CW:(kc + 1) * CW, :])
        g8 = fold(g24.T)
        gt[:, c * TB:(c + 1) * TB] = g8
        gs[c * TB:(c + 1) * TB, :] = wide(split3(g8), 24, TB).T.astype(BF16)

    pl.semaphore_wait(barrier, NUM_DEV - 1)
    x_pair = remote(x_hbm, xs_hbm, pair_s.at[0], pair_r.at[0], sib)
    x_pair.start()
    lab_pair = remote(lab_ref, lab_in, pair_s.at[1], pair_r.at[1], sib)
    lab_pair.start()

    def fwd(i, carry):
        fwd_block(i, False)
        return carry

    lax.fori_loop(1, NTB, fwd, 0)
    finish_prev(1, block_col(7))
    own = pl.ds(pl.multiple_of(core * TOK, TOK), TOK)
    st[:, own] += stx[...]
    st_pair = remote(st, st_in, pair_s.at[2], pair_r.at[2], sib)
    st_pair.start()
    for par in range(2):
        for nb in range(NBLK):
            a_store(par, nb, 0).wait()

    def a_load(j):
        return pltpu.make_async_copy(
            a_hbm.at[j], abuf.at[pl.ds(pl.multiple_of(lax.rem(j, 2) * 8, 8), 8)], ainsem.at[lax.rem(j, 2)])

    a_load(0).start()
    a_load(1).start()
    agt = w1.at[0:128]

    def resid_tile(tb):
        return wbuf.at[lax.rem(tb, 4), :, pl.ds(pl.multiple_of(tb // 4 * 128, 128), 128)]

    lane = lax.broadcasted_iota(jnp.int32, (NUM_TASKS, 128), 1)
    dgram = jnp.zeros((NUM_TASKS, 128), F32)
    for k in range(NUM_TASKS):
        dgram = jnp.where(lane == k, jnp.sum(diff * rolled(diff, k), axis=1, keepdims=True), dgram)
    lab_pair.wait_recv()
    st_pair.wait_recv()
    own_col = pl.multiple_of(core * TOK, TOK)
    sib_col = pl.multiple_of((1 - core) * TOK, TOK)

    def resid(col, labels):
        delta = st[:, pl.ds(col, TOK)] + st_in[:, pl.ds(col, TOK)]
        sign = jnp.where(labels == 0, -1.0, 1.0)
        u = sign * delta
        e = jnp.exp(-jnp.abs(u))
        return sign * (jnp.where(u >= 0, 1.0, e) / (1.0 + e)) * (1.0 / (TOK * NUM_DEV))

    ra = resid(own_col, lab_ref[...])
    rb = resid(sib_col, lab_in[...])
    first = core == 0
    rlo = jnp.where(first, ra, rb)
    rhi = jnp.where(first, rb, ra)
    cg = jnp.zeros((NUM_TASKS, 128), F32)
    for k in range(NUM_TASKS):
        prod = rlo * rolled(rlo, k) + rhi * rolled(rhi, k)
        cg = jnp.where(lane == k, jnp.sum(prod, axis=1, keepdims=True), cg)
    mrecv[chip] = cg

    def m_copy(m):
        dst = lax.rem(chip + m, NUM_CHIPS) * 2 + core
        return remote(mrecv.at[chip], mrecv.at[chip], msend.at[m - 1], mrec.at[m - 1], dst)

    for m in range(1, NUM_CHIPS):
        m_copy(m).start()

    for part, r in ((0, rlo), (1, rhi)):
        hi, mid, lo = split3(r)
        base = part * TOK
        r3[:, base:base + TOK] = jnp.concatenate([hi.astype(F32), mid.astype(F32), lo.astype(F32), jnp.zeros_like(r)], axis=0).astype(BF16)
        hf, mf, lf = hi.astype(F32), mid.astype(F32), lo.astype(F32)
        for c in range(TOK // TB):
            sl = slice(c * TB, (c + 1) * TB)
            stack = jnp.concatenate([hf[:, sl], hf[:, sl], mf[:, sl], hf[:, sl], lf[:, sl], mf[:, sl], jnp.zeros((80, TB), F32)], axis=0)
            wbuf[c, :, part * 128:(part + 1) * 128] = stack.T.astype(BF16)

    def slope_of(af):
        a2 = af * af
        th = jnp.tanh(af * (C0 + C1 * a2))
        h = 0.5 * af
        slope = (0.5 + 0.5 * th) + (h * (1.0 - th * th)) * (C0 + (3.0 * C1) * a2)
        return (h + h * th).astype(BF16), slope

    a_load(0).wait()

    def slope0(tb, tacc):
        pb, slope = slope_of(abuf[tb].astype(F32))
        for h in range(2):
            gbuf[12 + tb, h, :, :, :, 0:64] = slope[:, h * UW:(h + 1) * UW].reshape(2, 2, 2, 64, UW)
        return tacc + dot(r3[:, pl.ds(pl.multiple_of(tb * TB, TB), TB)], pb)

    tacc = lax.fori_loop(0, NTB, slope0, jnp.zeros((32, CW), F32))
    tref[:, 0:CW] = fold(tacc)

    for m in range(1, NUM_CHIPS):
        m_copy(m).wait_recv()
    mp = mrecv[0]
    for c in range(1, NUM_CHIPS):
        mp = mp + mrecv[c]
    mp = mp * dgram
    cols = [jnp.broadcast_to(mp[:, k:k + 1], (NUM_TASKS, 128)) for k in range(NUM_TASKS)]
    inv_scale = NUM_TASKS / sublane_sum(cols[0])

    def solve(step, w):
        ws = [rolled(w, k) for k in range(NUM_TASKS)]
        prods = [cols[k] * ws[k] for k in range(NUM_TASKS)]
        while len(ws) > 1:
            ws = [ws[i] + ws[i + 1] for i in range(0, len(ws), 2)]
            prods = [prods[i] + prods[i + 1] for i in range(0, len(prods), 2)]
        inv = 1.0 / ws[0]
        return (w * inv) * jnp.exp(-(prods[0] * inv) * inv_scale)

    wts = lax.fori_loop(0, SOLVER_STEPS, solve, jnp.full((NUM_TASKS, 128), 1.0 / NUM_TASKS, F32))
    wts = wts / sublane_sum(wts)
    mix_ref[...] = wts
    wcol = wts[:, 0:1]
    hi, mid, lo = [p.astype(F32) for p in split3(gt[...] * wcol)]
    agt[...] = jnp.concatenate([hi, mid, hi, lo, hi, mid, jnp.zeros((80, HALF), F32)], axis=0).astype(BF16)

    zl = lax.rem(cz, 2)
    zh = cz // 2
    to_x = me + 2 * (1 - 2 * cx)
    to_y = me + 4 * (1 - 2 * cy)
    to_zl = me + 8 * (1 - 2 * zl)
    to_zh = me + 16 * (1 - 2 * zh)
    pos1, pos2 = (cx, cy), (cy, cx)
    dev1, dev3 = (to_x, to_y), (to_y, to_x)

    def copy(j, h, s):
        u = 2 * j + h
        p1, p2 = pos1[h], pos2[h]
        if s < 2:
            zi = 1 - zl if s == 0 else zl
            src, dst, dev = gbuf.at[u, 1 - p1, zi], q1.at[u, zi], dev1[h]
        elif s == 2:
            src, dst, dev = gbuf.at[u, p1, 1 - zl], q2.at[u], to_zl
        elif s == 3:
            src, dst, dev = gbuf.at[u, p1, zl, 1 - p2], q3.at[u], dev3[h]
        else:
            src, dst, dev = gbuf.at[u, p1, zl, p2, 1 - zh], q4.at[u], to_zh
        return remote(src, dst, rsend.at[s, u], rrecv.at[s, u], dev)

    def out_cols(u):
        return pl.ds(pl.multiple_of(core * HALF + u * UW, UW), UW)

    def result(u, half):
        h = lax.rem(u, 2)
        p1 = (1 - h) * cx + h * cy
        p2 = (1 - h) * cy + h * cx
        return gbuf.at[u, p1, zl, p2, zh, pl.ds(pl.multiple_of(half * (ROWS // 2), 8), ROWS // 2)]

    def out_local(u):
        return pltpu.make_async_copy(result(u, core), up_hbm.at[:, out_cols(u)], fs_loc.at[u])

    def out_pair(u):
        return remote(result(u, 1 - core), up_hbm.at[:, out_cols(u)], fs.at[u], fv.at[u], sib)

    def stage(j, s):
        for h in range(2):
            u = 2 * j + h
            p1, p2 = pos1[h], pos2[h]
            if s == 2:
                copy(j, h, 0).wait_recv()
                gbuf[u, p1, 1 - zl] += q1[u, 1 - zl]
                copy(j, h, 2).start()
            elif s == 3:
                copy(j, h, 1).wait_recv()
                copy(j, h, 2).wait_recv()
                gbuf[u, p1, zl, 1 - p2] += q1[u, zl, 1 - p2] + q2[u, 1 - p2]
                copy(j, h, 3).start()
                gbuf[u, p1, zl, p2] += q1[u, zl, p2] + q2[u, p2]
            elif s == 4:
                copy(j, h, 3).wait_recv()
                gbuf[u, p1, zl, p2, 1 - zh] += q3[u, 1 - zh]
                copy(j, h, 4).start()
                gbuf[u, p1, zl, p2, zh] += q3[u, zh]
            else:
                copy(j, h, 4).wait_recv()
                gbuf[u, p1, zl, p2, zh] += q4[u]
                out_local(u).start()
                out_pair(u).start()

    def elem0(tb, carry):
        dp = dot(resid_tile(tb)[...], agt[:, 0:CW])
        for h in range(2):
            slope = gbuf[12 + tb, h, :, :, :, 0:64].reshape(TB, UW)
            da0[tb, :, h * UW:(h + 1) * UW] = (dp[:, h * UW:(h + 1) * UW] * slope).astype(BF16)
        return carry

    lax.fori_loop(0, NTB, elem0, 0)

    def block(j, cur, nxt):
        @pl.when(j < NBLK - 1)
        def _():
            a_load(j + 1).wait()

        @pl.when(j < NBLK - 2)
        def _():
            a_load(j + 2).start()

        ncol = pl.multiple_of(jnp.minimum(j + 1, NBLK - 1) * CW, CW)
        base = lax.rem(j + 1, 2) * 8

        def chunk(q, tacc):
            far = 1 - lax.rem(q, 2)
            xi = far * (1 - cx) + (1 - far) * cx
            near = q // 2
            zi = (1 - near) * (1 - zl) + near * zl
            g = dot(xt[zi, xi], cur[...].reshape(PAIR_TOK, CW)).reshape(2, 2, ROWS, CW)
            gbuf[2 * j, xi, zi] = g[:, :, :, :UW]
            for yi in range(2):
                gbuf[2 * j + 1, yi, zi, xi] = g[yi, :, :, UW:]
            for n in range(2):
                tb = 2 * q + n
                rows = pl.ds(pl.multiple_of(tb * TB, TB), TB)
                pb, slope = slope_of(abuf[base + tb].astype(F32))
                dp = dot(resid_tile(tb)[...], agt[:, pl.ds(ncol, CW)])
                nxt[tb] = (dp * slope).astype(BF16)
                tacc = tacc + dot(r3[:, rows], pb)

            for k, (h, part) in enumerate(((0, 0), (1, 0), (0, 1), (1, 1))):
                @pl.when(q == k)
                def _():
                    copy(j, h, part).start()

            for k, s, lag in PLAN:
                @pl.when((q == k) & (j >= lag))
                def _():
                    stage(j - lag, s)

            return tacc

        tacc = lax.fori_loop(0, 4, chunk, jnp.zeros((32, CW), F32))

        @pl.when(j < NBLK - 1)
        def _():
            tref[:, pl.ds(ncol, CW)] = fold(tacc)

    def two_blocks(jj, carry):
        block(2 * jj, da0, da1)
        block(2 * jj + 1, da1, da0)
        return carry

    lax.fori_loop(0, NBLK // 2, two_blocks, 0)

    for i in range(NUM_CHIPS):
        tp[i, :, 0:160] = tref[:, i * 160:(i + 1) * 160]

    def t_copy(i, src_chip):
        return remote(tp.at[i], trecv.at[src_chip], tsend.at[i], trec.at[src_chip], core * 16 + i)

    for i in range(NUM_CHIPS):
        @pl.when(core * 16 + i != me)
        def _():
            t_copy(i, chip).start()

        @pl.when(core * 16 + i == me)
        def _():
            trecv[chip] = tp[i]

    def late(b):
        for _, s, lag in PLAN:
            if b - lag < NBLK:
                stage(b - lag, s)

    late(NBLK)
    late(NBLK + 1)

    for c in range(NUM_CHIPS):
        @pl.when(c * 2 + me // 16 != me)
        def _():
            t_copy(0, c).wait_recv()

    tsum = trecv[0]
    for c in range(1, NUM_CHIPS):
        tsum = tsum + trecv[c]
    tsum_ref[...] = tsum
    ad_ref[...] = diff * wcol

    late(NBLK + 2)
    late(NBLK + 3)

    x_pair.wait_send()
    lab_pair.wait_send()
    st_pair.wait_send()
    for m in range(1, NUM_CHIPS):
        m_copy(m).wait_send()
    for i in range(NUM_CHIPS):
        @pl.when(core * 16 + i != me)
        def _():
            t_copy(i, chip).wait_send()

    def drain(j, carry):
        for h in range(2):
            for s in range(4):
                copy(j, h, s).wait_send()
        return carry

    def drain_out(j, carry):
        for h in range(2):
            copy(j, h, 4).wait_send()
            out_local(2 * j + h).wait()
            out_pair(2 * j + h).wait()
        return carry

    lax.fori_loop(0, NBLK, drain, 0)
    lax.fori_loop(0, NBLK - 3, drain_out, 0)
    late(NBLK + 4)
    late(NBLK + 5)
    lax.fori_loop(NBLK - 3, NBLK, drain_out, 0)


def place(mix_in, up_in, tsum_in, ad_in, mix_ref, up_hbm, down_hbm, ubuf, dbuf, sem):
    cols = [pl.ds(c * 1280, 1280) for c in range(4)]
    loads = [pltpu.make_async_copy(up_in.at[:, cu], ubuf.at[:, cu], sem.at[0, c]) for c, cu in enumerate(cols)]
    stores = [pltpu.make_async_copy(ubuf.at[:, cu], up_hbm.at[:, cu], sem.at[1, c]) for c, cu in enumerate(cols)]
    for cp in loads:
        cp.start()
    w = mix_in[...]
    diag = lax.broadcasted_iota(jnp.int32, w.shape, 0) == lax.broadcasted_iota(jnp.int32, w.shape, 1)
    mix_ref[...] = jnp.sum(jnp.where(diag, w, 0.0), axis=0)[:NUM_TASKS]
    down = lax.dot_general(tsum_in[...], ad_in[...], (((0,), (0,)), ((), ())), precision=lax.Precision.HIGHEST,
                           preferred_element_type=F32)
    dbuf[...] = down[:160]
    put = pltpu.make_async_copy(dbuf, down_hbm, sem.at[0, 4])
    put.start()
    for a, b in zip(loads, stores):
        a.wait()
        b.start()
    for cp in stores:
        cp.wait()
    put.wait()


def solution(mesh):
    def local_step(tok_rows, w_up, w_down, heads, label_rows):
        hc = jnp.transpose(heads, (0, 2, 1))
        vmem = pl.BlockSpec(memory_space=pltpu.VMEM)
        hbm = pl.BlockSpec(memory_space=pl.ANY)
        sds = jax.ShapeDtypeStruct
        dma = pltpu.SemaphoreType.DMA
        outs = pl.pallas_call(
            kernel,
            out_shape=(
                sds((NUM_TASKS, 128), F32),
                sds((40, HID), F32),
                sds((NUM_TASKS, 256), F32),
                sds((NUM_TASKS, DIM), F32),
                sds((NBLK, NTB, TB, CW), BF16),
                sds((TOK, DIM), BF16),
            ),
            in_specs=[hbm, hbm, hbm, vmem, vmem],
            out_specs=(vmem, hbm, vmem, vmem, hbm, hbm),
            scratch_shapes=[
                pltpu.VMEM((4, TB, DIM), BF16),
                pltpu.VMEM((DIM, HALF), BF16),
                pltpu.VMEM((2, 2, 4 * ROWS, PAIR_TOK), BF16),
                pltpu.VMEM((20, TB, CW), BF16),
                pltpu.VMEM((NTB, TB, CW), BF16),
                pltpu.VMEM((NTB, TB, CW), BF16),
                pltpu.VMEM((TB, 4 * TB), BF16),
                pltpu.VMEM((NUM_TASKS, TOK), F32),
                pltpu.VMEM((HALF, 128), BF16),
                pltpu.VMEM((NUM_TASKS, HALF), F32),
                pltpu.VMEM((DIM, 128), BF16),
                pltpu.VMEM((NUM_TASKS, PAIR_TOK), F32),
                pltpu.VMEM((NUM_TASKS, PAIR_TOK), F32),
                pltpu.VMEM((NUM_TASKS, TOK), jnp.int32),
                pltpu.VMEM((32, PAIR_TOK), BF16),
                pltpu.VMEM((NUM_TASKS, HALF), F32),
                pltpu.VMEM((NUM_CHIPS, NUM_TASKS, 256), F32),
                pltpu.VMEM((NUM_CHIPS, NUM_TASKS, 256), F32),
                pltpu.VMEM((NUM_CHIPS, NUM_TASKS, 128), F32),
                pltpu.VMEM((NUNIT, 2, 2, 2, 2, ROWS, UW), F32),
                pltpu.VMEM((NUNIT, 2, 2, 2, ROWS, UW), F32),
                pltpu.VMEM((NUNIT, 2, 2, ROWS, UW), F32),
                pltpu.VMEM((NUNIT, 2, ROWS, UW), F32),
                pltpu.VMEM((NUNIT, ROWS, UW), F32),
                dma((25,)), dma((5,)), dma((4,)), dma((2, NBLK)), dma((2,)),
                dma((3,)), dma((3,)), dma((15,)), dma((15,)), dma((16,)), dma((16,)),
                dma((5, NUNIT)), dma((5, NUNIT)), dma((NUNIT,)), dma((NUNIT,)), dma((NUNIT,)),
            ],
            compiler_params=pltpu.CompilerParams(
                collective_id=0, has_side_effects=True, vmem_limit_bytes=67043328),
        )(tok_rows, w_up, w_down, hc, label_rows)
        return pl.pallas_call(
            place,
            out_shape=(sds((NUM_TASKS,), F32), sds((40, HID), F32), sds((160, DIM), F32)),
            in_specs=[vmem, hbm, vmem, vmem],
            out_specs=(vmem, hbm, hbm),
            scratch_shapes=[pltpu.VMEM((40, HID), F32), pltpu.VMEM((160, DIM), F32), dma((2, 5))],
        )(*outs[:4])

    return jax.shard_map(
        local_step, mesh=mesh, in_specs=(P('data', None), P(), P(), P(), P(None, 'data')),
        out_specs=(P(), P('data', None), P('data', None)), check_vma=False)
```
